32 devices in a mesh: sweep: 1 (over z), ent: 32 (over y, x, core).
Axes of the slice: x: 4, y: 4, z: 1, core: 2. Of those that a mesh axis runs over, the one named last changes fastest.
The devices are a block of a 4x4x8 slice.
Arguments:
- ent_emb: float32 [262144, 200], P(('sweep', 'ent'))
- ent_ada: float32 [262144], P(('sweep', 'ent'))
- rel_emb: float32 [237, 200], P('sweep')
- rel_ada: float32 [237], P('sweep')
- head_idx: int32 [32, 16, 2048], P(('sweep', 'ent'))
- tail_idx: int32 [32, 16, 2048], P(('sweep', 'ent'))
- rel_idx: int32 [32, 16, 2048], P(('sweep', 'ent'))
- edge_mask: int32 [32, 16, 2048], P(('sweep', 'ent'))
- neg_idx: int32 [16, 500], P('sweep')
Outputs:
- output 1: float32 [262144, 200], P(('sweep', 'ent'))
- output 2: float32 [262144], P(('sweep', 'ent'))
- output 3: float32 [237, 200], P('sweep')
- output 4: float32 [237], P('sweep')
- output 5: float32 [32, 16], P(('sweep', 'ent'))
All inputs are finite; a program needn't handle non-finite values.
Results may differ from the reference program's by a relative error of at most 0.001.
Values are sent between devices in bfloat16 or wider.
A program may use at most 768 MiB of HBM per device.

```python
import jax
import jax.numpy as jnp
from jax import lax

ENT_DEVS = 32
PART_ROWS = 8192
EMB_DIM = 200
NUM_REL = 237
NEG_COUNT = 500
EDGE_COUNT = 2048
ROUNDS = 16
TABLE_ROWS = ENT_DEVS * PART_ROWS
LEARN_RATE = 0.05
ADA_EPS = 1e-10


def draw_index(rng_key, upper, out_shape):
    key_a, key_b, key_c = jax.random.split(rng_key, 3)
    plain_ids = jax.random.randint(key_a, out_shape, 0, upper)
    hot_ids = jax.random.randint(key_b, out_shape, 0, max(upper // 16, 1))
    hot_pick = jax.random.randint(key_c, out_shape, 0, 4)
    return jnp.where(hot_pick == 0, hot_ids, plain_ids).astype(jnp.int32)


def setup_inputs(seed: int = 0, part: int = 0) -> dict:
    part_key = jax.random.fold_in(jax.random.key(seed), part)
    keys = jax.random.split(part_key, 10)
    rel_hits = EDGE_COUNT * ENT_DEVS / NUM_REL
    bucket = (ENT_DEVS, ROUNDS, EDGE_COUNT)
    fill_count = jax.random.randint(keys[7], (ENT_DEVS, ROUNDS, 1), EDGE_COUNT // 8, EDGE_COUNT + 1)
    return {
        'ent_emb': jax.random.normal(keys[0], (TABLE_ROWS, EMB_DIM), jnp.float32) * EMB_DIM ** -0.25,
        'ent_ada': jax.random.uniform(keys[1], (TABLE_ROWS,), jnp.float32, 0.5, 1.5) * EMB_DIM ** -0.5,
        'rel_emb': jax.random.normal(keys[2], (NUM_REL, EMB_DIM), jnp.float32) * 0.5 ** 0.5,
        'rel_ada': jax.random.uniform(keys[3], (NUM_REL,), jnp.float32, 0.5, 1.5) * (0.5 * rel_hits / EMB_DIM),
        'head_idx': draw_index(keys[4], PART_ROWS, bucket),
        'tail_idx': draw_index(keys[5], PART_ROWS, bucket),
        'rel_idx': jax.random.randint(keys[6], bucket, 0, NUM_REL).astype(jnp.int32),
        'edge_mask': (jax.random.randint(keys[8], bucket, 0, EDGE_COUNT) < fill_count).astype(jnp.int32),
        'neg_idx': jax.random.randint(keys[9], (ROUNDS, NEG_COUNT), 0, TABLE_ROWS).astype(jnp.int32),
    }


def bucket_grads(head_rows, tail_rows, neg_rows, rel_rows, edge_w):
    half = head_rows.shape[-1] // 2
    head_f = head_rows.astype(jnp.float32)
    h_re = head_f[:, :half]
    h_im = head_f[:, half:]
    r_re = rel_rows[:, :half]
    r_im = rel_rows[:, half:]
    query = jnp.concatenate([h_re * r_re - h_im * r_im, h_re * r_im + h_im * r_re], axis=1)
    query_bf = query.astype(jnp.bfloat16)
    tail_f = tail_rows.astype(jnp.float32)
    pos_score = jnp.sum(query * tail_f, axis=1)
    neg_score = jnp.dot(query_bf, neg_rows.T, preferred_element_type=jnp.float32)
    top_score = jnp.maximum(pos_score, jnp.max(neg_score, axis=1))
    pos_exp = jnp.exp(pos_score - top_score)
    neg_exp = jnp.exp(neg_score - top_score[:, None])
    norm_sum = pos_exp + jnp.sum(neg_exp, axis=1)
    log_norm = top_score + jnp.log(norm_sum)
    loss = jnp.sum(edge_w * (log_norm - pos_score)) / EDGE_COUNT
    pos_grad = edge_w * (pos_exp / norm_sum - 1.0)
    neg_grad = (edge_w[:, None] * neg_exp / norm_sum[:, None]).astype(jnp.bfloat16)
    query_grad = pos_grad[:, None] * tail_f + jnp.dot(neg_grad, neg_rows, preferred_element_type=jnp.float32)
    tail_grad = pos_grad[:, None] * query
    negrow_grad = jnp.dot(neg_grad.T, query_bf, preferred_element_type=jnp.float32)
    g_re = query_grad[:, :half]
    g_im = query_grad[:, half:]
    head_grad = jnp.concatenate([g_re * r_re + g_im * r_im, g_im * r_re - g_re * r_im], axis=1)
    relrow_grad = jnp.concatenate([g_re * h_re + g_im * h_im, g_im * h_re - g_re * h_im], axis=1)
    return loss, head_grad, tail_grad, negrow_grad, relrow_grad


def adagrad_rows(table, state, grad):
    new_state = state + jnp.mean(grad * grad, axis=1)
    return table - LEARN_RATE * grad / jnp.sqrt(new_state + ADA_EPS)[:, None], new_state


def reference(ent_emb, ent_ada, rel_emb, rel_ada, head_idx, tail_idx, rel_idx, edge_mask, neg_idx):
    def train_step(carry, round_no):
        table, state, rel_tab, rel_state = carry
        table_bf = table.astype(jnp.bfloat16)
        neg_ids = neg_idx[round_no]
        neg_rows = table_bf[neg_ids]

        def one_bucket(acc_pair, dev_no):
            grad_ent, grad_rel = acc_pair
            head_ids = dev_no * PART_ROWS + head_idx[dev_no, round_no]
            tail_ids = ((dev_no + round_no) % ENT_DEVS) * PART_ROWS + tail_idx[dev_no, round_no]
            rel_ids = rel_idx[dev_no, round_no]
            edge_w = edge_mask[dev_no, round_no].astype(jnp.float32)
            loss, head_grad, tail_grad, negrow_grad, relrow_grad = bucket_grads(
                table_bf[head_ids], table_bf[tail_ids], neg_rows, rel_tab[rel_ids], edge_w)
            grad_ent = grad_ent.at[head_ids].add(head_grad).at[tail_ids].add(tail_grad).at[neg_ids].add(negrow_grad)
            grad_rel = grad_rel.at[rel_ids].add(relrow_grad)
            return (grad_ent, grad_rel), loss

        zero_acc = (jnp.zeros_like(table), jnp.zeros_like(rel_tab))
        (grad_ent, grad_rel), losses = lax.scan(one_bucket, zero_acc, jnp.arange(ENT_DEVS))
        table, state = adagrad_rows(table, state, grad_ent)
        rel_tab, rel_state = adagrad_rows(rel_tab, rel_state, grad_rel)
        return (table, state, rel_tab, rel_state), losses

    init_carry = (ent_emb, ent_ada, rel_emb, rel_ada)
    (table, state, rel_tab, rel_state), losses = lax.scan(train_step, init_carry, jnp.arange(ROUNDS))
    return table, state, rel_tab, rel_state, losses.T
```

```python
import functools

import jax
import jax.numpy as jnp
from jax import lax
from jax.experimental import pallas as pl
from jax.experimental.pallas import tpu as pltpu
from jax.sharding import PartitionSpec as P

LEARN_RATE = 0.05
ADA_EPS = 1e-10
LANES = 128
CHUNK = 256
PACK_ROWS = 1024
F32, BF16, I32 = jnp.float32, jnp.bfloat16, jnp.int32
MESH = pl.DeviceIdType.MESH
VMEM = pltpu.VMEM


def round_up(value, multiple):
    return -(-value // multiple) * multiple


class Dims:
    def __init__(self, mesh, ent_emb, rel_emb, head_idx, neg_idx):
        self.ent = mesh.shape['ent']
        self.chips = self.ent // 2
        self.rows, self.dim = ent_emb.shape
        self.half = self.dim // 2
        self.hp = round_up(self.half, 8)
        self.dc = 2 * self.hp
        self.num_rel = rel_emb.shape[0]
        self.relp = round_up(self.num_rel, LANES)
        self.rounds, self.edges = head_idx.shape[1:]
        self.nch = self.edges // CHUNK
        self.neg = neg_idx.shape[1]
        self.negp = round_up(self.neg, self.ent * 16)
        self.negc = self.negp // self.ent
        self.cols = (self.relp + self.negp) // LANES
        self.tiles = self.dc // 8 * self.cols
        self.tpd = -(-self.tiles // self.ent)
        self.trows = 2 * self.rows + 16


def nt_dot(lhs, rhs):
    return lax.dot_general(lhs, rhs, (((1,), (1,)), ((), ())), preferred_element_type=F32)


def nn_dot(lhs, rhs):
    return jnp.dot(lhs, rhs, preferred_element_type=F32)


def split3(x):
    hi = x.astype(BF16)
    rest = x - hi.astype(F32)
    mid = rest.astype(BF16)
    lo = (rest - mid.astype(F32)).astype(BF16)
    return hi, mid, lo


def iota(shape, dim):
    return lax.broadcasted_iota(I32, shape, dim)


def eye(n):
    return jnp.where(iota((n, n), 0) == iota((n, n), 1), 1.0, 0.0).astype(BF16)


def compact_sel(dims, out_rows):
    c = iota((out_rows, 2 * LANES), 0)
    lane = iota((out_rows, 2 * LANES), 1)
    src = jnp.where(c < dims.hp, c, c - dims.hp + LANES)
    return jnp.where((lane == src) & (c < dims.dc), 1.0, 0.0).astype(BF16)


def pack_kernel(half, last, e_ref, g_ref, o_ref):
    step = pl.program_id(0)
    lane = iota((LANES, LANES), 1)

    @pl.when(step < last)
    def _():
        g_cols = jnp.transpose(g_ref[...])
        for i in range(PACK_ROWS // LANES):
            rows = pl.ds(i * LANES, LANES)
            lo = e_ref[rows, :LANES]
            hi = e_ref[rows, LANES:]
            shift = LANES - half
            im = jnp.where(lane < shift, pltpu.roll(lo, shift, 1), pltpu.roll(hi, shift, 1))
            im = jnp.where(lane < half, im, 0.0)
            im = jnp.where(lane == LANES - 1, g_cols[:, i:i + 1], im)
            o_ref[pl.ds(2 * i * LANES, LANES, stride=2), :] = jnp.where(lane < half, lo, 0.0)
            o_ref[pl.ds(2 * i * LANES + 1, LANES, stride=2), :] = im

    @pl.when(step == last)
    def _():
        o_ref[...] = jnp.zeros_like(o_ref)


def pack(dims, emb, ada):
    blocks = dims.rows // PACK_ROWS
    return pl.pallas_call(
        functools.partial(pack_kernel, dims.half, blocks),
        grid=(blocks + 1,),
        out_shape=jax.ShapeDtypeStruct((dims.trows, LANES), F32),
        in_specs=[pl.BlockSpec((PACK_ROWS, 2 * LANES), lambda i: (jnp.minimum(i, blocks - 1), 0)),
                  pl.BlockSpec((PACK_ROWS // LANES, LANES), lambda i: (jnp.minimum(i, blocks - 1), 0))],
        out_specs=pl.BlockSpec((2 * PACK_ROWS, LANES), lambda i: (i, 0)),
        name='pack')(emb, ada.reshape(dims.rows // LANES, LANES))


def unpack_kernel(half, t_ref, e_ref, g_ref):
    lane = iota((LANES, LANES), 1)
    g_cols = jnp.zeros((LANES, LANES), F32)
    for i in range(PACK_ROWS // LANES):
        rows = pl.ds(i * LANES, LANES)
        re = t_ref[pl.ds(2 * i * LANES, LANES, stride=2), :]
        im = t_ref[pl.ds(2 * i * LANES + 1, LANES, stride=2), :]
        im_hi = pltpu.roll(im, half, 1)
        e_ref[rows, :LANES] = jnp.where(lane < half, re, im_hi)
        e_ref[rows, LANES:] = im_hi
        g_cols = jnp.where(lane == i, im[:, LANES - 1:], g_cols)
    g_ref[...] = jnp.transpose(g_cols)[:PACK_ROWS // LANES, :]


def unpack(dims, table):
    blocks = dims.rows // PACK_ROWS
    emb, ada = pl.pallas_call(
        functools.partial(unpack_kernel, dims.half),
        grid=(blocks,),
        out_shape=[jax.ShapeDtypeStruct((dims.rows, dims.dim), F32),
                   jax.ShapeDtypeStruct((dims.rows // LANES, LANES), F32)],
        in_specs=[pl.BlockSpec((2 * PACK_ROWS, LANES), lambda i: (i, 0))],
        out_specs=[pl.BlockSpec((PACK_ROWS, 2 * LANES), lambda i: (i, 0)),
                   pl.BlockSpec((PACK_ROWS // LANES, LANES), lambda i: (i, 0))],
        name='unpack')(table)
    return emb, ada.reshape(dims.rows)


def index_kernel(dims, x_ref, o_ref, send_sem, recv_sem):
    me = lax.axis_index('ent')
    barrier = pltpu.get_barrier_semaphore()
    for s in range(1, dims.rounds):
        pl.semaphore_signal(barrier, inc=1, device_id={'ent': lax.rem(me + dims.ent - s, dims.ent)}, device_id_type=MESH)
    pl.semaphore_wait(barrier, dims.rounds - 1)
    copies = [pltpu.make_async_remote_copy(
        src_ref=x_ref.at[s], dst_ref=o_ref.at[s], send_sem=send_sem.at[s], recv_sem=recv_sem.at[s],
        device_id={'ent': lax.rem(me + s, dims.ent)}, device_id_type=MESH) for s in range(1, dims.rounds)]
    for copy in copies:
        copy.start()
    o_ref[0] = x_ref[0]
    for copy in copies:
        copy.wait()


def exchange_indices(dims, both):
    return pl.pallas_call(
        functools.partial(index_kernel, dims),
        out_shape=jax.ShapeDtypeStruct(both.shape, I32),
        in_specs=[pl.BlockSpec(memory_space=VMEM)], out_specs=pl.BlockSpec(memory_space=VMEM),
        scratch_shapes=[pltpu.SemaphoreType.DMA((dims.rounds,))] * 2,
        name='index_exchange',
        compiler_params=pltpu.CompilerParams(collective_id=0, has_side_effects=True))(both)


UNROLL_SCATTER = 16
UNROLL_GATHER = 64
UPDATE_ROWS = 64


def table_kernel(dims, old, new, head_ids, tail_ids, neg_ids, *refs):
    refs = list(refs)
    if old is not None:
        head_g, tail_g, neg_g = refs[:3]
        refs = refs[3:]
    table_in = refs.pop(0)
    if old is not None:
        table = refs.pop(0)
    else:
        table = table_in
    if new is not None:
        head_out, tail_out, neg_out = refs[:3]
        refs = refs[3:]
    ids, sem = refs[:2]
    refs = refs[2:]
    if old is not None:
        acc_a, acc_b = refs[:2]
        refs = refs[2:]
    if new is not None:
        stage, = refs

    edges, negp = dims.edges, dims.negp
    copies = []
    for base, step in ((0, old), (1, new)):
        if step is not None:
            for k, (src, size) in enumerate(((head_ids, edges), (tail_ids, edges), (neg_ids, negp))):
                copies.append(pltpu.make_async_copy(src.at[pl.ds(step * size, size)], ids[3 * base + k], sem.at[3 * base + k]))
    for copy in copies:
        copy.start()

    if old is not None:
        def zero(c, _):
            rows = pl.ds(pl.multiple_of(c * 128, 128), 128)
            acc_a[rows, :] = jnp.zeros((128, LANES), F32)
            acc_b[rows, :] = jnp.zeros((128, LANES), F32)
            return 0
        lax.fori_loop(0, 2 * dims.rows // 128, zero, 0)
    for copy in copies:
        copy.wait()

    def pair(k):
        return pl.ds(pl.multiple_of(2 * k, 2), 2)

    def at(ref, k):
        return pl.ds(pl.multiple_of(ref[k], 2), 2)

    if old is not None:
        old_h, old_t, old_n = ids[:3]

        def scatter(c, _):
            for u in range(UNROLL_SCATTER):
                k = c * UNROLL_SCATTER + u
                h, t = at(old_h, k), at(old_t, k)
                new_a = acc_a[h, :] + head_g[pair(k), :]
                new_b = acc_b[t, :] + tail_g[pair(k), :]
                acc_a[h, :] = new_a
                acc_b[t, :] = new_b
            return 0
        lax.fori_loop(0, edges // UNROLL_SCATTER, scatter, 0)

        def scatter_neg(c, _):
            for u in range(UNROLL_SCATTER // 2):
                k = c * UNROLL_SCATTER + 2 * u
                h, t = at(old_n, k), at(old_n, k + 1)
                new_a = acc_a[h, :] + neg_g[pair(k), :]
                new_b = acc_b[t, :] + neg_g[pair(k + 1), :]
                acc_a[h, :] = new_a
                acc_b[t, :] = new_b
            return 0
        lax.fori_loop(0, negp // UNROLL_SCATTER, scatter_neg, 0)

        lane = iota((UPDATE_ROWS, LANES), 1)

        def update(c, _):
            re = pl.ds(pl.multiple_of(c * 2 * UPDATE_ROWS, 2 * UPDATE_ROWS), UPDATE_ROWS, stride=2)
            im = pl.ds(pl.multiple_of(c * 2 * UPDATE_ROWS, 2 * UPDATE_ROWS) + 1, UPDATE_ROWS, stride=2)
            g_re = acc_a[re, :] + acc_b[re, :]
            g_im = acc_a[im, :] + acc_b[im, :]
            e_re, e_im = table_in[re, :], table_in[im, :]
            part = (g_re * g_re + g_im * g_im) * (1.0 / dims.dim)
            part = jnp.where(lane == LANES - 1, e_im, part)
            state = jnp.sum(part, axis=1, keepdims=True)
            rate = LEARN_RATE / jnp.sqrt(state + ADA_EPS)
            table[re, :] = e_re - rate * g_re
            table[im, :] = jnp.where(lane == LANES - 1, state, e_im - rate * g_im)
            return 0
        lax.fori_loop(0, dims.rows // UPDATE_ROWS, update, 0)
        table[pl.ds(2 * dims.rows, 16), :] = jnp.zeros((16, LANES), F32)

    if new is not None:
        new_h, new_t, new_n = ids[3:]
        sel = compact_sel(dims, 2 * LANES)

        def gather(ref, count):
            def body(c, _):
                for u in range(UNROLL_GATHER):
                    k = c * UNROLL_GATHER + u
                    stage[pair(k), :] = table[at(ref, k), :]
                return 0
            lax.fori_loop(0, count // UNROLL_GATHER, body, 0)

        def staged(c):
            re = stage[pl.ds(pl.multiple_of(c * 2 * CHUNK, 2 * CHUNK), CHUNK, stride=2), :]
            im = stage[pl.ds(pl.multiple_of(c * 2 * CHUNK, 2 * CHUNK) + 1, CHUNK, stride=2), :]
            return jnp.concatenate([re.astype(BF16), im.astype(BF16)], axis=1)

        for ref, out in ((new_t, tail_out), (new_h, head_out)):
            gather(ref, edges)

            def convert(c, _):
                out[c] = nt_dot(sel[:dims.dc], staged(c)).astype(BF16)
                return 0
            lax.fori_loop(0, dims.nch, convert, 0)
        gather(new_n, negp)
        for c in range(negp // CHUNK):
            rows = nt_dot(staged(c), sel).astype(BF16)
            neg_out[pl.ds(c * CHUNK, CHUNK), :] = rows


def table_step(dims, old, new, ids, grads, table):
    vm = pl.BlockSpec(memory_space=VMEM)
    anys = pl.BlockSpec(memory_space=pl.ANY)
    in_specs = [anys] * 3
    operands = list(ids)
    outs, aliases = [], {}
    smem = lambda n: pltpu.SMEM((n,), I32)
    sizes = (dims.edges, dims.edges, dims.negp)
    if old is not None:
        in_specs += [vm] * 3
        operands += list(grads)
        aliases = {len(operands): 0}
        outs.append(jax.ShapeDtypeStruct((dims.trows, LANES), F32))
    in_specs.append(vm)
    operands.append(table)
    if new is not None:
        outs += [jax.ShapeDtypeStruct((dims.nch, dims.dc, CHUNK), BF16)] * 2
        outs.append(jax.ShapeDtypeStruct((dims.negp, 2 * LANES), BF16))
    id_scratch = [smem(n) for n in sizes] * 2
    scratch = [pltpu.SemaphoreType.DMA((6,))]
    if old is not None:
        scratch += [VMEM((dims.trows, LANES), F32)] * 2
    if new is not None:
        scratch += [VMEM((2 * dims.edges, LANES), F32)]

    def body(*refs):
        n = len(operands) + len(outs)
        table_kernel(dims, old, new, *refs[:n], refs[n:n + 6], *refs[n + 6:])

    res = pl.pallas_call(
        body, out_shape=outs, in_specs=in_specs, out_specs=[vm] * len(outs),
        scratch_shapes=id_scratch + scratch, input_output_aliases=aliases,
        name=f'table_{"x" if old is None else "u"}{"x" if new is None else "g"}',
        compiler_params=pltpu.CompilerParams(vmem_limit_bytes=34 << 20))(*operands)
    return res


def bucket_kernel(dims, s, head, tail, neg, rel_t, rel_state, rel_ids, rel_ids_p, weight,
                  head_g, tail_g, neg_g, rel_t_out, rel_state_out, loss,
                  tail_r, head_r, dp_s, dp_r, splits, qb, dsb, neg_p, neg_half, neg_buf, neg_acc, neg_all, neg_t,
                  acc_rel, acc_neg, head_c, x_ar, p_ar, half_ar, buf_ar, acc_ar, o_ar,
                  tail_ss, tail_rs, head_ss, head_rs, one_s, one_r, rs_s, rs_r, ag_s, ag_r, rs2_s, rs2_r, ag2_s, ag2_r):
    ent, chips, hp, dc, nch = dims.ent, dims.chips, dims.hp, dims.dc, dims.nch
    me = lax.axis_index('ent')
    core, chip = lax.rem(me, 2), me // 2
    partner = me + 1 - 2 * core
    dst_t = lax.rem(me + ent - s, ent)
    dst_h = lax.rem(me + s, ent)

    def dev(d):
        return {'ent': d}

    def peer(k):
        return lax.rem(chip + k, chips) * 2 + core

    def remote(src, dst, ss, rs, d):
        return pltpu.make_async_remote_copy(src_ref=src, dst_ref=dst, send_sem=ss, recv_sem=rs, device_id=dev(d), device_id_type=MESH)

    barrier = pltpu.get_barrier_semaphore()

    def signal(k, _):
        pl.semaphore_signal(barrier, inc=1, device_id=dev(peer(k)), device_id_type=MESH)
        return 0
    pl.semaphore_signal(barrier, inc=1, device_id=dev(partner), device_id_type=MESH)
    if s:
        pl.semaphore_signal(barrier, inc=1, device_id=dev(dst_t), device_id_type=MESH)
        pl.semaphore_signal(barrier, inc=1, device_id=dev(dst_h), device_id_type=MESH)
    lax.fori_loop(1, chips, signal, 0)

    for i, part in enumerate(split3(rel_t[...])):
        splits[pl.ds(i * dc, dc), :] = part
    qb[pl.ds(dc, 2 * LANES - dc), :] = jnp.zeros((2 * LANES - dc, CHUNK), BF16)
    acc_rel[...] = jnp.zeros_like(acc_rel)
    acc_neg[...] = jnp.zeros_like(acc_neg)
    loss[...] = jnp.zeros_like(loss)
    ident = eye(CHUNK)

    pl.semaphore_wait(barrier, chips + (2 if s else 0))

    def tail_copy(c):
        return remote(tail.at[c], tail_r.at[c], tail_ss.at[c], tail_rs.at[c], dst_t)

    def head_copy(c):
        return remote(head.at[c], head_r.at[c], head_ss.at[c], head_rs.at[c], dst_h)

    def loop(lo, hi, fn):
        def body(k, _):
            fn(k)
            return 0
        lax.fori_loop(lo, hi, body, 0)

    neg_pair = remote(neg.at[1 - core], neg_p, one_s.at[0], one_r.at[0], partner)
    neg_pair.start()
    if s:
        loop(0, nch, lambda c: tail_copy(c).start())
        loop(0, nch, lambda c: head_copy(c).start())
        tail_in, head_in, dp_in = tail_r, head_r, dp_r
    else:
        tail_in, head_in, dp_in = tail, head, dp_s

    neg_pair.wait_recv()
    neg_half[...] = neg[core] + neg_p[...]

    def rs_neg(k):
        return remote(neg_half.at[lax.rem(chip + k, chips)], neg_buf.at[k], rs_s.at[k], rs_r.at[k], peer(k))
    loop(1, chips, lambda k: rs_neg(k).start())
    neg_acc[...] = neg_half[chip]

    def take_neg(k):
        rs_neg(k).wait_recv()
        neg_acc[...] = neg_acc[...] + neg_buf[k]
    loop(1, chips, take_neg)

    def ag_neg(k):
        return remote(neg_acc, neg_all.at[core, chip], ag_s.at[k], ag_r.at[k], peer(k))
    loop(1, chips, lambda k: ag_neg(k).start())
    neg_all[core, chip] = neg_acc[...]
    loop(1, chips, lambda k: ag_neg(k).wait_recv())
    neg_pair2 = remote(neg_all.at[core], neg_all.at[core], one_s.at[1], one_r.at[1], partner)
    neg_pair2.start()
    neg_pair2.wait_recv()
    neg_rows = neg_all[...].reshape(dims.negp, 2 * LANES)
    neg_t[...] = nt_dot(eye(2 * LANES), neg_rows).astype(BF16)

    def one_hot(ids_ref, c):
        ids = ids_ref[pl.ds(s * nch + c, 1), :]
        return jnp.where(iota((dims.relp, CHUNK), 0) == ids, 1.0, 0.0).astype(BF16)

    def rel_rows(hot):
        r = nn_dot(splits[...], hot)
        r = (r[:dc] + r[dc:2 * dc]) + r[2 * dc:]
        return r[:hp], r[hp:]

    def queries(rows, r_re, r_im):
        x = rows.astype(F32)
        h_re, h_im = x[:hp], x[hp:]
        return h_re, h_im, h_re * r_re - h_im * r_im, h_re * r_im + h_im * r_re

    def head_side(c):
        hot = one_hot(rel_ids, c)
        r_re, r_im = rel_rows(hot)
        h_re, h_im, q_re, q_im = queries(head[c], r_re, r_im)
        qb[pl.ds(0, dc), :] = jnp.concatenate([q_re, q_im], axis=0).astype(BF16)
        scores = nn_dot(neg_all[...].reshape(dims.negp, 2 * LANES), qb[...])
        scores = jnp.where(iota((dims.negp, CHUNK), 0) < dims.neg, scores, -1e30)
        if s:
            tail_copy(c).wait_recv()
        t = tail_in[c].astype(F32)
        t_re, t_im = t[:hp], t[hp:]
        pos = jnp.sum(q_re * t_re + q_im * t_im, axis=0, keepdims=True)
        top = jnp.maximum(pos, jnp.max(scores, axis=0, keepdims=True))
        pos_exp = jnp.exp(pos - top)
        neg_exp = jnp.exp(scores - top)
        norm = pos_exp + jnp.sum(neg_exp, axis=0, keepdims=True)
        w = weight[pl.ds(s * nch + c, 1), :]
        loss[pl.ds(0, 1), :] += w * (top + jnp.log(norm) - pos)
        dp = w * (pos_exp / norm - 1.0)
        dp_s[pl.ds(c, 1), :] = dp
        dsb[...] = (neg_exp * (w / norm)).astype(BF16)
        mix = nn_dot(neg_t[pl.ds(0, dc), :], dsb[...])
        g_re = dp * t_re + mix[:hp]
        g_im = dp * t_im + mix[hp:]
        acc_neg[...] += nt_dot(qb[pl.ds(0, dc), :], dsb[...])
        head_c[c] = jnp.concatenate([g_re * r_re + g_im * r_im, g_im * r_re - g_re * r_im], axis=0)
        rel_g = jnp.concatenate([g_re * h_re + g_im * h_im, g_im * h_re - g_re * h_im], axis=0)
        acc_rel[...] += nt_dot(jnp.concatenate(split3(rel_g), axis=1), jnp.concatenate([hot] * 3, axis=1))
    loop(0, nch, head_side)

    if s:
        dp_copy = remote(dp_s, dp_r, one_s.at[2], one_r.at[2], dst_h)
        dp_copy.start()

    def tile_place(t):
        d, j = t // dims.tpd, t % dims.tpd
        return d // chips, d % chips, j
    rel_cols = dims.relp // LANES
    for t in range(dims.tpd * ent):
        i, j = t // dims.cols, t % dims.cols
        if t >= dims.tiles:
            x_ar[tile_place(t)] = jnp.zeros((8, LANES), F32)
        elif j < rel_cols:
            x_ar[tile_place(t)] = acc_rel[pl.ds(8 * i, 8), pl.ds(j * LANES, LANES)]
        else:
            x_ar[tile_place(t)] = acc_neg[pl.ds(8 * i, 8), pl.ds((j - rel_cols) * LANES, LANES)]

    ar_pair = remote(x_ar.at[1 - core], p_ar, one_s.at[3], one_r.at[3], partner)
    ar_pair.start()

    def rows_of(cols):
        gap = jnp.zeros((LANES - hp, CHUNK), F32)
        x = jnp.concatenate([cols[:hp], gap, cols[hp:], gap], axis=0)
        return nt_dot(jnp.concatenate([ident] * 3, axis=1), jnp.concatenate(split3(x), axis=1))

    def put_rows(out, c, rows):
        base = pl.multiple_of(c * 2 * CHUNK, 2 * CHUNK)
        out[pl.ds(base, CHUNK, stride=2), :] = rows[:, :LANES]
        out[pl.ds(base + 1, CHUNK, stride=2), :] = rows[:, LANES:]

    def head_rows(c):
        put_rows(head_g, c, rows_of(head_c[c]))

    def tail_side(c):
        if s:
            head_copy(c).wait_recv()
        r_re, r_im = rel_rows(one_hot(rel_ids_p, c))
        _, _, q_re, q_im = queries(head_in[c], r_re, r_im)
        put_rows(tail_g, c, rows_of(dp_in[pl.ds(c, 1), :] * jnp.concatenate([q_re, q_im], axis=0)))

    ar_pair.wait_recv()
    half_ar[...] = x_ar[core] + p_ar[...]

    def rs_ar(k):
        return remote(half_ar.at[lax.rem(chip + k, chips)], buf_ar.at[k], rs2_s.at[k], rs2_r.at[k], peer(k))
    loop(1, chips, lambda k: rs_ar(k).start())
    loop(0, nch, head_rows)
    acc_ar[...] = half_ar[chip]

    def take_ar(k):
        rs_ar(k).wait_recv()
        acc_ar[...] += buf_ar[k]
    loop(1, chips, take_ar)

    def ag_ar(k):
        return remote(acc_ar, o_ar.at[core, chip], ag2_s.at[k], ag2_r.at[k], peer(k))
    loop(1, chips, lambda k: ag_ar(k).start())
    o_ar[core, chip] = acc_ar[...]
    if s:
        dp_copy.wait_recv()
    loop(0, nch, tail_side)
    loop(1, chips, lambda k: ag_ar(k).wait_recv())
    ar_pair2 = remote(o_ar.at[core], o_ar.at[core], one_s.at[4], one_r.at[4], partner)
    ar_pair2.start()
    ar_pair2.wait_recv()

    for t in range(dims.tiles):
        i, j = t // dims.cols, t % dims.cols
        if j < rel_cols:
            acc_rel[pl.ds(8 * i, 8), pl.ds(j * LANES, LANES)] = o_ar[tile_place(t)]
        else:
            acc_neg[pl.ds(8 * i, 8), pl.ds((j - rel_cols) * LANES, LANES)] = o_ar[tile_place(t)]
    g = acc_rel[...]
    state = rel_state[...] + jnp.sum(g * g, axis=0, keepdims=True) * (1.0 / dims.dim)
    rel_state_out[...] = state
    rel_t_out[...] = rel_t[...] - LEARN_RATE * g / jnp.sqrt(state[:1] + ADA_EPS)
    for c in range(dims.negp // CHUNK):
        put_rows(neg_g, c, rows_of(acc_neg[:, pl.ds(c * CHUNK, CHUNK)]))

    neg_pair.wait_send()
    neg_pair2.wait_send()
    ar_pair.wait_send()
    ar_pair2.wait_send()
    if s:
        dp_copy.wait_send()

        def sent(c):
            tail_copy(c).wait_send()
            head_copy(c).wait_send()
        loop(0, nch, sent)

    def sent_peers(k):
        rs_neg(k).wait_send()
        ag_neg(k).wait_send()
        rs_ar(k).wait_send()
        ag_ar(k).wait_send()
    loop(1, chips, sent_peers)


def bucket_step(dims, s, head, tail, neg, rel_t, rel_state, rel_ids, rel_ids_p, weight):
    d = dims
    vm = pl.BlockSpec(memory_space=VMEM)
    sds = jax.ShapeDtypeStruct
    dma = pltpu.SemaphoreType.DMA
    outs = [sds((2 * d.edges, LANES), F32), sds((2 * d.edges, LANES), F32), sds((2 * d.negp, LANES), F32),
            sds((d.dc, d.relp), F32), sds((8, d.relp), F32), sds((8, CHUNK), F32)]
    rows = VMEM((d.nch, d.dc, CHUNK), BF16)
    neg_part = VMEM((d.chips, d.negc, 2 * LANES), BF16)
    ar_part = VMEM((d.chips, d.tpd, 8, LANES), F32)
    scratch = [rows, rows, VMEM((d.nch, CHUNK), F32), VMEM((d.nch, CHUNK), F32),
               VMEM((3 * d.dc, d.relp), BF16), VMEM((2 * LANES, CHUNK), BF16), VMEM((d.negp, CHUNK), BF16),
               neg_part, neg_part, neg_part, VMEM((d.negc, 2 * LANES), BF16),
               VMEM((2, d.chips, d.negc, 2 * LANES), BF16), VMEM((2 * LANES, d.negp), BF16),
               VMEM((d.dc, d.relp), F32), VMEM((d.dc, d.negp), F32), VMEM((d.nch, d.dc, CHUNK), F32),
               VMEM((2, d.chips, d.tpd, 8, LANES), F32), ar_part, ar_part, ar_part,
               VMEM((d.tpd, 8, LANES), F32), VMEM((2, d.chips, d.tpd, 8, LANES), F32),
               dma((d.nch,)), dma((d.nch,)), dma((d.nch,)), dma((d.nch,)), dma((5,)), dma((5,))]
    scratch += [dma((d.chips,))] * 8
    return pl.pallas_call(
        functools.partial(bucket_kernel, d, s), out_shape=outs, in_specs=[vm] * 8, out_specs=[vm] * 6,
        scratch_shapes=scratch, name=f'bucket_{s}',
        compiler_params=pltpu.CompilerParams(collective_id=1 + s, has_side_effects=True, vmem_limit_bytes=30 << 20),
    )(head, tail, neg.reshape(2, d.chips, d.negc, 2 * LANES), rel_t, rel_state, rel_ids, rel_ids_p, weight)


def solution(mesh):
    row_spec = P(('sweep', 'ent'), None)
    flat_spec = P(('sweep', 'ent'))
    rel_spec = P('sweep', None)
    state_spec = P('sweep')
    edge_spec = P(('sweep', 'ent'), None, None)

    def device_fn(ent_emb, ent_ada, rel_emb, rel_ada, head_idx, tail_idx, rel_idx, edge_mask, neg_idx):
        d = Dims(mesh, ent_emb, rel_emb, head_idx, neg_idx)
        me = lax.axis_index('ent')
        table = pack(d, ent_emb, ent_ada)
        rel = jnp.pad(rel_emb.reshape(d.num_rel, 2, d.half), ((0, d.relp - d.num_rel), (0, 0), (0, d.hp - d.half)))
        rel_t = rel.reshape(d.relp, d.dc).T
        rel_state = jnp.broadcast_to(jnp.pad(rel_ada, (0, d.relp - d.num_rel), constant_values=1.0), (8, d.relp))

        both = jnp.stack([tail_idx[0], rel_idx[0]], axis=1).reshape(d.rounds, 2 * d.edges // LANES, LANES)
        both = exchange_indices(d, both).reshape(d.rounds, 2, d.edges)
        head_ids = (head_idx[0] * 2).reshape(-1)
        tail_ids = (both[:, 0] * 2).reshape(-1)
        local = neg_idx - me * d.rows
        owned = (local >= 0) & (local < d.rows)
        neg_ids = jnp.where(owned, local, d.rows) * 2
        neg_ids = jnp.pad(neg_ids, ((0, 0), (0, d.negp - d.neg)), constant_values=2 * d.rows).reshape(-1)
        ids = (head_ids, tail_ids, neg_ids)
        rel_ids = rel_idx[0].reshape(d.rounds * d.nch, CHUNK)
        rel_ids_p = both[:, 1].reshape(d.rounds * d.nch, CHUNK)
        weight = edge_mask[0].astype(F32).reshape(d.rounds * d.nch, CHUNK)

        head, tail, neg = table_step(d, None, 0, ids, None, table)
        losses = []
        for s in range(d.rounds):
            hg, tg, ng, rel_t, rel_state, loss = bucket_step(d, s, head, tail, neg, rel_t, rel_state, rel_ids, rel_ids_p, weight)
            losses.append(loss[0])
            last = s == d.rounds - 1
            res = table_step(d, s, None if last else s + 1, ids, (hg, tg, ng), table)
            table = res[0]
            if not last:
                head, tail, neg = res[1:]
        loss = jnp.sum(jnp.stack(losses), axis=1) / d.edges
        emb, ada = unpack(d, table)
        rel_out = rel_t.T.reshape(d.relp, 2, d.hp)[:d.num_rel, :, :d.half].reshape(d.num_rel, d.dim)
        return emb, ada, rel_out, rel_state[0, :d.num_rel], loss[None, :]

    return jax.shard_map(device_fn, mesh=mesh,
                         in_specs=(row_spec, flat_spec, rel_spec, state_spec, edge_spec, edge_spec, edge_spec, edge_spec, rel_spec),
                         out_specs=(row_spec, flat_spec, rel_spec, state_spec, row_spec), check_vma=False)
```

```python
import functools

import jax
import jax.numpy as jnp
from jax import lax
from jax.experimental import pallas as pl
from jax.experimental.pallas import tpu as pltpu
from jax.sharding import PartitionSpec as P

LEARN_RATE = 0.05
ADA_EPS = 1e-10
LANES = 128
CHUNK = 256
PACK_ROWS = 1024
QUERY_GROUP, SCORE_GROUP, HEAD_GROUP, ROWS_GROUP, TAIL_GROUP = 2, 2, 2, 4, 2
TAILS_FIRST = 2
AHEAD = 2
HEAD_SENDS = {0: (0, 2, 3, 4, 5, 7, 8), **{k: (4, 8, 8, 8, 8, 8, 8) for k in (1, 2, 3, 6, 7, 8)}}
F32, BF16, I32 = jnp.float32, jnp.bfloat16, jnp.int32
MESH = pl.DeviceIdType.MESH
VMEM = pltpu.VMEM


def round_up(value, multiple):
    return -(-value // multiple) * multiple


class Dims:
    def __init__(self, mesh, ent_emb, rel_emb, head_idx, neg_idx):
        self.ent = mesh.shape['ent']
        self.chips = self.ent // 2
        self.rows, self.dim = ent_emb.shape
        self.half = self.dim // 2
        self.hp = round_up(self.half, 8)
        self.dc = 2 * self.hp
        self.num_rel = rel_emb.shape[0]
        self.relp = round_up(self.num_rel, LANES)
        self.rounds, self.edges = head_idx.shape[1:]
        self.nch = self.edges // CHUNK
        self.neg = neg_idx.shape[1]
        self.negp = round_up(self.neg, self.ent * 16)
        self.negc = self.negp // self.ent
        self.cols = (self.relp + self.negp) // LANES
        self.tiles = self.dc // 8 * self.cols
        self.tpd = -(-self.tiles // self.ent)
        self.trows = 2 * self.rows + 16


def nt_dot(lhs, rhs):
    return lax.dot_general(lhs, rhs, (((1,), (1,)), ((), ())), preferred_element_type=F32)


def nn_dot(lhs, rhs):
    return jnp.dot(lhs, rhs, preferred_element_type=F32)


def split3(x):
    hi = x.astype(BF16)
    rest = x - hi.astype(F32)
    mid = rest.astype(BF16)
    lo = (rest - mid.astype(F32)).astype(BF16)
    return hi, mid, lo


def iota(shape, dim):
    return lax.broadcasted_iota(I32, shape, dim)


def eye(n):
    return jnp.where(iota((n, n), 0) == iota((n, n), 1), 1.0, 0.0).astype(BF16)


def compact_sel(dims, out_rows):
    c = iota((out_rows, 2 * LANES), 0)
    lane = iota((out_rows, 2 * LANES), 1)
    src = jnp.where(c < dims.hp, c, c - dims.hp + LANES)
    return jnp.where((lane == src) & (c < dims.dc), 1.0, 0.0).astype(BF16)


def pack_kernel(half, last, e_ref, g_ref, o_ref):
    step = pl.program_id(0)
    row = iota((LANES, LANES), 0)
    low = half // 8 * 8
    gap = jnp.zeros((LANES - round_up(half, 8), LANES), F32)

    @pl.when(step < last)
    def _():
        for i in range(PACK_ROWS // LANES):
            cols = pl.ds(i * LANES, LANES)
            re = jnp.concatenate([e_ref[pl.ds(0, round_up(half, 8)), cols], gap], axis=0)
            re = jnp.where(row < half, re, 0.0)
            im = jnp.concatenate([e_ref[pl.ds(low, 2 * half - low), cols], jnp.zeros((LANES - (2 * half - low), LANES), F32)], axis=0)
            if half > low:
                im = pltpu.roll(im, LANES - (half - low), 0)
            im = jnp.where(row < half, im, 0.0)
            im = jnp.where(row == LANES - 1, g_ref[pl.ds(i, 1), :], im)
            o_ref[pl.ds(2 * i * LANES, LANES, stride=2), :] = jnp.transpose(re)
            o_ref[pl.ds(2 * i * LANES + 1, LANES, stride=2), :] = jnp.transpose(im)

    @pl.when(step == last)
    def _():
        o_ref[...] = jnp.zeros_like(o_ref)


def pack(dims, emb, ada):
    blocks = dims.rows // PACK_ROWS
    return pl.pallas_call(
        functools.partial(pack_kernel, dims.half, blocks),
        grid=(blocks + 1,),
        out_shape=jax.ShapeDtypeStruct((dims.trows, LANES), F32),
        in_specs=[pl.BlockSpec((dims.dim, PACK_ROWS), lambda i: (0, jnp.minimum(i, blocks - 1))),
                  pl.BlockSpec((PACK_ROWS // LANES, LANES), lambda i: (jnp.minimum(i, blocks - 1), 0))],
        out_specs=pl.BlockSpec((2 * PACK_ROWS, LANES), lambda i: (i, 0)),
        compiler_params=pltpu.CompilerParams(vmem_limit_bytes=16 << 20),
        name='pack')(emb.T, ada.reshape(dims.rows // LANES, LANES))


def unpack_kernel(half, t_ref, e_ref, g_ref):
    low = half // 8 * 8
    high = round_up(half, 8)
    for i in range(PACK_ROWS // LANES):
        cols = pl.ds(i * LANES, LANES)
        re = jnp.transpose(t_ref[pl.ds(2 * i * LANES, LANES, stride=2), :])
        im = jnp.transpose(t_ref[pl.ds(2 * i * LANES + 1, LANES, stride=2), :])
        g_ref[pl.ds(i, 1), :] = im[LANES - 1:]
        e_ref[pl.ds(0, low), cols] = re[:low]
        if half > low:
            im = pltpu.roll(im, half - low, 0)
            e_ref[pl.ds(low, 8), cols] = jnp.where(iota((8, LANES), 0) < half - low, re[low:high], im[:8])
            e_ref[pl.ds(high, 2 * half - high), cols] = im[8:8 + 2 * half - high]
        else:
            e_ref[pl.ds(half, half), cols] = im[:half]


def unpack(dims, table):
    blocks = dims.rows // PACK_ROWS
    emb, ada = pl.pallas_call(
        functools.partial(unpack_kernel, dims.half),
        grid=(blocks,),
        out_shape=[jax.ShapeDtypeStruct((dims.dim, dims.rows), F32),
                   jax.ShapeDtypeStruct((dims.rows // LANES, LANES), F32)],
        in_specs=[pl.BlockSpec((2 * PACK_ROWS, LANES), lambda i: (i, 0))],
        out_specs=[pl.BlockSpec((dims.dim, PACK_ROWS), lambda i: (0, i)),
                   pl.BlockSpec((PACK_ROWS // LANES, LANES), lambda i: (i, 0))],
        compiler_params=pltpu.CompilerParams(vmem_limit_bytes=16 << 20),
        name='unpack')(table)
    return emb.T, ada.reshape(dims.rows)


UNROLL_SCATTER = 16
UNROLL_GATHER = 64
UNROLL_NEG = 8
GATHER_GROUP = 4
UPDATE_ROWS = 512


def table_kernel(dims, update_rows, gather_next, *refs):
    refs = list(refs)

    def take(n):
        taken = refs[:n]
        del refs[:n]
        return taken
    edges, negp = dims.edges, dims.negp
    sources, lists = [], []
    if update_rows:
        old_count, = take(1)
        sources += take(4)
    if gather_next:
        new_count, = take(1)
        sources += take(4)
    if update_rows:
        head_g, tail_g, neg_g = take(3)
    table_in, = take(1)
    table, = take(1) if update_rows else (table_in,)
    if gather_next:
        tail_out, head_out, neg_out = take(3)
    lists = take(len(sources))
    sem, = take(1)
    if update_rows:
        acc_a, acc_b = take(2)
    if gather_next:
        stage, = take(1)
    copies = [pltpu.make_async_copy(src, dst, sem.at[k]) for k, (src, dst) in enumerate(zip(sources, lists))]
    for copy in copies:
        copy.start()
    if update_rows:
        head_i, tail_i, neg_i, src_i = lists[:4]
        table_update(dims, copies, old_count, head_i, tail_i, neg_i, src_i, head_g, tail_g, neg_g, table_in, table, acc_a, acc_b)
    else:
        for copy in copies:
            copy.wait()
    if gather_next:
        head_i, tail_i, neg_i, src_i = lists[-4:]
        sel = compact_sel(dims, 2 * LANES)

        def staged(c):
            base = pl.multiple_of(c * 2 * CHUNK, 2 * CHUNK)
            re = stage[pl.ds(base, CHUNK, stride=2), :]
            im = stage[pl.ds(base + 1, CHUNK, stride=2), :]
            return jnp.concatenate([re.astype(BF16), im.astype(BF16)], axis=1)

        for ids, out in ((tail_i, tail_out), (head_i, head_out)):
            def gather(c, _):
                for u in range(UNROLL_GATHER):
                    k = c * UNROLL_GATHER + u
                    stage[pair(k), :] = table[at(ids, k), :]
                return 0
            lax.fori_loop(0, edges // UNROLL_GATHER, gather, 0)

            def convert(c, _):
                for u in range(GATHER_GROUP):
                    k = c * GATHER_GROUP + u
                    out[k] = nt_dot(sel[:dims.dc], staged(k)).astype(BF16)
                return 0
            lax.fori_loop(0, dims.nch // GATHER_GROUP, convert, 0)

        stage[pl.ds(0, 2 * negp), :] = jnp.zeros((2 * negp, LANES), F32)

        def gather_neg(c, _):
            rows = [table[at(neg_i, c * UNROLL_NEG + u), :] for u in range(UNROLL_NEG)]
            for u in range(UNROLL_NEG):
                stage[at(src_i, c * UNROLL_NEG + u), :] = rows[u]
            return 0
        lax.fori_loop(0, (new_count[0] + UNROLL_NEG - 1) // UNROLL_NEG, gather_neg, 0)
        for c in range(negp // CHUNK):
            neg_out[pl.ds(c * CHUNK, CHUNK), :] = nt_dot(staged(c), sel).astype(BF16)


def table_update(dims, copies, count, head_i, tail_i, neg_i, src_i, head_g, tail_g, neg_g, table_in, table, acc_a, acc_b):
    edges = dims.edges

    def zero(c, _):
        rows = pl.ds(pl.multiple_of(c * 256, 256), 256)
        acc_a[rows, :] = jnp.zeros((256, LANES), F32)
        acc_b[rows, :] = jnp.zeros((256, LANES), F32)
        return 0
    lax.fori_loop(0, 2 * dims.rows // 256, zero, 0)
    for copy in copies:
        copy.wait()

    def scatter(c, _):
        for u in range(0, UNROLL_SCATTER, 2):
            k = c * UNROLL_SCATTER + u
            h0, h1, t0, t1 = at(head_i, k), at(head_i, k + 1), at(tail_i, k), at(tail_i, k + 1)
            a0 = acc_a[h0, :] + head_g[pair(k), :]
            b0 = acc_b[t0, :] + tail_g[pair(k), :]
            a1 = jnp.where(head_i[k] == head_i[k + 1], a0, acc_a[h1, :]) + head_g[pair(k + 1), :]
            b1 = jnp.where(tail_i[k] == tail_i[k + 1], b0, acc_b[t1, :]) + tail_g[pair(k + 1), :]
            acc_a[h0, :] = a0
            acc_b[t0, :] = b0
            acc_a[h1, :] = a1
            acc_b[t1, :] = b1
        return 0
    lax.fori_loop(0, edges // UNROLL_SCATTER, scatter, 0)

    def scatter_neg(c, _):
        for u in range(0, UNROLL_NEG, 2):
            k = c * UNROLL_NEG + u
            h, t = at(neg_i, k), at(neg_i, k + 1)
            new_a = acc_a[h, :] + neg_g[at(src_i, k), :]
            new_b = acc_b[t, :] + neg_g[at(src_i, k + 1), :]
            acc_a[h, :] = new_a
            acc_b[t, :] = new_b
        return 0
    lax.fori_loop(0, (count[0] + UNROLL_NEG - 1) // UNROLL_NEG, scatter_neg, 0)

    lane = iota((UPDATE_ROWS, LANES), 1)

    def update(c, _):
        base = pl.multiple_of(c * 2 * UPDATE_ROWS, 2 * UPDATE_ROWS)
        re = pl.ds(base, UPDATE_ROWS, stride=2)
        im = pl.ds(base + 1, UPDATE_ROWS, stride=2)
        g_re = acc_a[re, :] + acc_b[re, :]
        g_im = acc_a[im, :] + acc_b[im, :]
        e_re, e_im = table_in[re, :], table_in[im, :]
        part = (g_re * g_re + g_im * g_im) * (1.0 / dims.dim)
        part = jnp.where(lane == LANES - 1, e_im, part)
        state = jnp.sum(part, axis=1, keepdims=True)
        rate = LEARN_RATE * lax.rsqrt(state + ADA_EPS)
        table[re, :] = e_re - rate * g_re
        table[im, :] = jnp.where(lane == LANES - 1, state, e_im - rate * g_im)
        return 0
    lax.fori_loop(0, dims.rows // UPDATE_ROWS, update, 0)
    table[pl.ds(2 * dims.rows, 16), :] = jnp.zeros((16, LANES), F32)


def pair(k):
    return pl.ds(pl.multiple_of(2 * k, 2), 2)


def at(ref, k):
    return pl.ds(pl.multiple_of(ref[k], 2), 2)


def table_step(dims, old, new, grads, table):
    vm = pl.BlockSpec(memory_space=VMEM)
    smem = pl.BlockSpec(memory_space=pltpu.SMEM)
    anys = pl.BlockSpec(memory_space=pl.ANY)
    sizes = (dims.edges, dims.edges, dims.negp, dims.negp)
    operands, in_specs, outs, scratch, aliases = [], [], [], [], {}
    for lists in (old, new):
        if lists is not None:
            operands += lists
            in_specs += [smem] + [anys] * 4
            scratch += [pltpu.SMEM((n,), I32) for n in sizes]
    scratch.append(pltpu.SemaphoreType.DMA((len(scratch),)))
    if old is not None:
        operands += grads
        in_specs += [vm] * 3
        aliases = {len(operands): 0}
        outs.append(jax.ShapeDtypeStruct((dims.trows, LANES), F32))
        scratch += [VMEM((dims.trows, LANES), F32)] * 2
    operands.append(table)
    in_specs.append(vm)
    if new is not None:
        outs += [jax.ShapeDtypeStruct((dims.nch, dims.dc, CHUNK), BF16)] * 2
        outs.append(jax.ShapeDtypeStruct((dims.negp, 2 * LANES), BF16))
        scratch.append(VMEM((2 * dims.edges, LANES), F32))
    return pl.pallas_call(
        functools.partial(table_kernel, dims, old is not None, new is not None),
        out_shape=outs, in_specs=in_specs, out_specs=[vm] * len(outs), scratch_shapes=scratch,
        input_output_aliases=aliases, name='table',
        compiler_params=pltpu.CompilerParams(vmem_limit_bytes=24 << 20))(*operands)


def bucket_kernel(dims, s, *refs):
    (head, tail, neg, rel_t, rel_state, rel_ids, rel_ids_p, weight), refs = refs[:8], refs[8:]
    if s == 0:
        (tail_x, rel_x), refs = refs[:2], refs[2:]
    (head_g, tail_g, neg_g, rel_t_out, rel_state_out, loss), refs = refs[:6], refs[6:]
    if s == 0:
        rel_x_out, tail_x_out = refs[0], refs[1:dims.rounds]
        refs = refs[dims.rounds:]
        (x_ss, x_rs), refs = refs[:2], refs[2:]
    (tail_r, head_r, dp_s, dp_r, splits, q_all, r_all, qb, ex, top_s, sum_s, neg_p, neg_half, neg_buf, neg_acc, neg_all, neg_t,
     acc_rel, acc_neg, head_c, x_ar, p_ar, half_ar, buf_ar, acc_ar, o_ar,
     tail_ss, tail_rs, head_ss, head_rs, one_s, one_r, rs_s, rs_r, ag_s, ag_r, rs2_s, rs2_r, ag2_s, ag2_r) = refs
    ent, chips, hp, dc, nch = dims.ent, dims.chips, dims.hp, dims.dc, dims.nch
    me = lax.axis_index('ent')
    core, chip = lax.rem(me, 2), me // 2
    partner = me + 1 - 2 * core
    dst_t = lax.rem(me + ent - s, ent)
    dst_h = lax.rem(me + s, ent)

    def dev(d):
        return {'ent': d}

    def peer(k):
        return lax.rem(chip + k, chips) * 2 + core

    def remote(src, dst, ss, rs, d):
        return pltpu.make_async_remote_copy(src_ref=src, dst_ref=dst, send_sem=ss, recv_sem=rs, device_id=dev(d), device_id_type=MESH)

    def loop(lo, hi, fn):
        def body(k, _):
            fn(k)
            return 0
        lax.fori_loop(lo, hi, body, 0)

    def chunks(group, fn):
        loop(0, nch // group, lambda k: fn([k * group + i for i in range(group)]))

    barrier = pltpu.get_barrier_semaphore()

    def signal(d):
        pl.semaphore_signal(barrier, inc=1, device_id=dev(d), device_id_type=MESH)
    if s:
        signal(dst_t)
        signal(dst_h)
        others = 2
    else:
        loop(1, dims.rounds, lambda k: signal(lax.rem(me + ent - k, ent)))
        others = dims.rounds - 1
    loop(1, chips, lambda k: signal(peer(k)))
    signal(partner)

    def one_hot(ids_ref, c):
        ids = ids_ref[pl.ds(s * nch + c, 1), :]
        return jnp.where(iota((dims.relp, CHUNK), 0) == ids, 1.0, 0.0).astype(BF16)

    def rel_rows(hot):
        r = nn_dot(splits[...], hot)
        return (r[:dc] + r[dc:2 * dc]) + r[2 * dc:]

    def queries(rows, r):
        x = rows.astype(F32)
        h_re, h_im, r_re, r_im = x[:hp], x[hp:], r[:hp], r[hp:]
        return jnp.concatenate([h_re * r_re - h_im * r_im, h_re * r_im + h_im * r_re], axis=0)

    def rel_query(cs):
        for c in cs:
            r_all[c] = rel_rows(one_hot(rel_ids, c))

    def head_query(cs):
        for c in cs:
            q = queries(head[c], r_all[c])
            q_all[c] = q
            qb[c, pl.ds(0, dc), :] = q.astype(BF16)

    ident = eye(CHUNK)
    for c in range(nch):
        qb[c, pl.ds(dc, 2 * LANES - dc), :] = jnp.zeros((2 * LANES - dc, CHUNK), BF16)
    acc_rel[...] = jnp.zeros_like(acc_rel)
    acc_neg[...] = jnp.zeros_like(acc_neg)
    loss[...] = jnp.zeros_like(loss)
    pl.semaphore_wait(barrier, chips + others)

    def tail_copy(c):
        return remote(tail.at[c], tail_r.at[c], tail_ss.at[c], tail_rs.at[c], dst_t)

    def head_copy(c):
        return remote(head.at[c], head_r.at[c], head_ss.at[c], head_rs.at[c], dst_h)

    def send_tails(lo, hi):
        if s:
            loop(lo, hi, lambda c: tail_copy(c).start())

    def send_heads(lo, hi):
        if s and hi > lo:
            loop(lo, hi, lambda c: head_copy(c).start())
    plan = (0,) + HEAD_SENDS.get(s, HEAD_SENDS[0])
    late = s > 0 and plan[2] < nch

    def send_heads_at(point):
        if point < 2:
            send_heads(plan[point], plan[point + 1])
        elif s:
            for c in range(plan[point], plan[point + 1]):
                if c >= AHEAD:
                    head_copy(c - AHEAD).wait_send()
                head_copy(c).start()
    if s:
        tail_in, head_in, dp_in = tail_r, head_r, dp_r
    else:
        tail_in, head_in, dp_in = tail, head, dp_s

    first = GATHER_GROUP
    send_tails(0, TAILS_FIRST)
    neg_pair = remote(neg.at[1 - core], neg_p, one_s.at[0], one_r.at[0], partner)
    neg_pair.start()
    neg_pair.wait_recv()
    neg_half[...] = neg[core] + neg_p[...]

    def rs_neg(k):
        return remote(neg_half.at[lax.rem(chip + k, chips)], neg_buf.at[k], rs_s.at[k], rs_r.at[k], peer(k))
    loop(1, chips, lambda k: rs_neg(k).start())
    send_tails(TAILS_FIRST, first)
    send_heads_at(0)
    neg_acc[...] = neg_half[chip]

    def take_neg(k):
        rs_neg(k).wait_recv()
        neg_acc[...] = neg_acc[...] + neg_buf[k]
    loop(1, chips, take_neg)

    def ag_neg(k):
        return remote(neg_acc, neg_all.at[core, chip], ag_s.at[k], ag_r.at[k], peer(k))
    loop(1, chips, lambda k: ag_neg(k).start())
    send_tails(first, nch)
    send_heads_at(1)
    if s == 0:
        def rel_copy(k):
            rows = pl.ds(pl.multiple_of(k * nch, nch), nch)
            return remote(rel_x.at[rows], rel_x_out.at[rows], x_ss.at[0, k], x_rs.at[0, k], lax.rem(me + k, ent))

        def id_copy(k):
            return remote(tail_x.at[pl.ds(k * dims.edges, dims.edges)], tail_x_out[k - 1], x_ss.at[1, k], x_rs.at[1, k], lax.rem(me + k, ent))
        loop(1, dims.rounds, lambda k: rel_copy(k).start())
        for k in range(1, dims.rounds):
            id_copy(k).start()
        rel_x_out[pl.ds(0, nch), :] = rel_x[pl.ds(0, nch), :]
    for i, part in enumerate(split3(rel_t[...])):
        splits[pl.ds(i * dc, dc), :] = part
    chunks(QUERY_GROUP, rel_query)
    chunks(QUERY_GROUP, head_query)
    neg_all[core, chip] = neg_acc[...]
    loop(1, chips, lambda k: ag_neg(k).wait_recv())
    neg_pair2 = remote(neg_all.at[core], neg_all.at[core], one_s.at[1], one_r.at[1], partner)
    neg_pair2.start()
    neg_pair2.wait_recv()
    neg_t[...] = nt_dot(eye(2 * LANES), neg_all[...].reshape(dims.negp, 2 * LANES)).astype(BF16)

    main = dims.neg // 16 * 16

    def score(cs):
        for c in cs:
            scores = nn_dot(neg_all[...].reshape(dims.negp, 2 * LANES), qb[c])
            body = scores[:main]
            top = jnp.max(body, axis=0, keepdims=True)
            if main < dims.negp:
                rest = jnp.where(iota((dims.negp - main, CHUNK), 0) < dims.neg - main, scores[main:], -1e30)
                top = jnp.maximum(top, jnp.max(rest, axis=0, keepdims=True))
            e_body = jnp.exp(body - top)
            ex[c, pl.ds(0, main), :] = e_body
            total = jnp.sum(e_body, axis=0, keepdims=True)
            if main < dims.negp:
                e_rest = jnp.exp(rest - top)
                ex[c, pl.ds(main, dims.negp - main), :] = e_rest
                total = total + jnp.sum(e_rest, axis=0, keepdims=True)
            top_s[pl.ds(c, 1), :] = top
            sum_s[pl.ds(c, 1), :] = total
    chunks(SCORE_GROUP, score)

    def head_side(cs):
        if s:
            for c in cs:
                tail_copy(c).wait_recv()
        lost, neg_q, neg_d, rel_parts, rel_hot = [], [], [], [], []
        for c in cs:
            t = tail_in[c].astype(F32)
            pos = jnp.sum(q_all[c] * t, axis=0, keepdims=True)
            neg_top = top_s[pl.ds(c, 1), :]
            top = jnp.maximum(pos, neg_top)
            pos_exp = jnp.exp(pos - top)
            scale = jnp.exp(neg_top - top)
            norm = pos_exp + scale * sum_s[pl.ds(c, 1), :]
            w = weight[pl.ds(s * nch + c, 1), :]
            lost.append(w * (top + jnp.log(norm) - pos))
            dp = w * (pos_exp / norm - 1.0)
            dp_s[pl.ds(c, 1), :] = dp
            ds = (ex[c] * (w * scale / norm)).astype(BF16)
            g = dp * t + nn_dot(neg_t[pl.ds(0, dc), :], ds)
            neg_q.append(qb[c, pl.ds(0, dc), :])
            neg_d.append(ds)
            g_re, g_im = g[:hp], g[hp:]
            r = r_all[c]
            r_re, r_im = r[:hp], r[hp:]
            head_c[c] = jnp.concatenate([g_re * r_re + g_im * r_im, g_im * r_re - g_re * r_im], axis=0)
            h = head[c].astype(F32)
            h_re, h_im = h[:hp], h[hp:]
            rel_g = jnp.concatenate([g_re * h_re + g_im * h_im, g_im * h_re - g_re * h_im], axis=0)
            rel_parts.append(jnp.concatenate(split3(rel_g), axis=0))
            rel_hot.append(one_hot(rel_ids, c))
        loss[pl.ds(0, 1), :] += sum(lost)
        acc_neg[...] += nt_dot(jnp.concatenate(neg_q, axis=1), jnp.concatenate(neg_d, axis=1))
        part = nt_dot(jnp.concatenate(rel_parts, axis=1), jnp.concatenate(rel_hot, axis=1))
        acc_rel[...] += (part[:dc] + part[dc:2 * dc]) + part[2 * dc:]
    chunks(HEAD_GROUP, head_side)

    if s:
        dp_copy = remote(dp_s, dp_r, one_s.at[2], one_r.at[2], dst_h)
        dp_copy.start()

    def tile_place(t):
        d, j = t // dims.tpd, t % dims.tpd
        return d // chips, d % chips, j
    rel_cols = dims.relp // LANES
    for t in range(dims.tpd * ent):
        i, j = t // dims.cols, t % dims.cols
        if t >= dims.tiles:
            x_ar[tile_place(t)] = jnp.zeros((8, LANES), F32)
        elif j < rel_cols:
            x_ar[tile_place(t)] = acc_rel[pl.ds(8 * i, 8), pl.ds(j * LANES, LANES)]
        else:
            x_ar[tile_place(t)] = acc_neg[pl.ds(8 * i, 8), pl.ds((j - rel_cols) * LANES, LANES)]

    ar_pair = remote(x_ar.at[1 - core], p_ar, one_s.at[3], one_r.at[3], partner)
    ar_pair.start()
    send_heads_at(2)

    def rows_of(cols):
        gap = jnp.zeros((LANES - hp, CHUNK), F32)
        x = jnp.concatenate([cols[:hp], gap, cols[hp:], gap], axis=0)
        return nt_dot(jnp.concatenate([ident] * 3, axis=1), jnp.concatenate(split3(x), axis=1))

    def put_rows(out, c, rows):
        base = pl.multiple_of(c * 2 * CHUNK, 2 * CHUNK)
        out[pl.ds(base, CHUNK, stride=2), :] = rows[:, :LANES]
        out[pl.ds(base + 1, CHUNK, stride=2), :] = rows[:, LANES:]

    def head_rows(cs):
        for c in cs:
            put_rows(head_g, c, rows_of(head_c[c]))

    def tail_side(cs):
        if s:
            for c in cs:
                head_copy(c).wait_recv()
        for c in cs:
            q = queries(head_in[c], rel_rows(one_hot(rel_ids_p, c)))
            put_rows(tail_g, c, rows_of(dp_in[pl.ds(c, 1), :] * q))

    ar_pair.wait_recv()
    half_ar[...] = x_ar[core] + p_ar[...]

    def rs_ar(k):
        return remote(half_ar.at[lax.rem(chip + k, chips)], buf_ar.at[k], rs2_s.at[k], rs2_r.at[k], peer(k))
    loop(1, chips, lambda k: rs_ar(k).start())
    send_heads_at(3)
    chunks(ROWS_GROUP, head_rows)
    send_heads_at(4)
    acc_ar[...] = half_ar[chip]

    def take_ar(k):
        rs_ar(k).wait_recv()
        acc_ar[...] += buf_ar[k]
    loop(1, chips, take_ar)

    def ag_ar(k):
        return remote(acc_ar, o_ar.at[core, chip], ag2_s.at[k], ag2_r.at[k], peer(k))
    loop(1, chips, lambda k: ag_ar(k).start())
    send_heads_at(5)
    o_ar[core, chip] = acc_ar[...]
    def tail_gradients():
        if s:
            dp_copy.wait_recv()
        chunks(TAIL_GROUP, tail_side)
    if not late:
        tail_gradients()
    loop(1, chips, lambda k: ag_ar(k).wait_recv())
    ar_pair2 = remote(o_ar.at[core], o_ar.at[core], one_s.at[4], one_r.at[4], partner)
    ar_pair2.start()
    send_heads_at(6)
    ar_pair2.wait_recv()

    for t in range(dims.tiles):
        i, j = t // dims.cols, t % dims.cols
        if j < rel_cols:
            acc_rel[pl.ds(8 * i, 8), pl.ds(j * LANES, LANES)] = o_ar[tile_place(t)]
        else:
            acc_neg[pl.ds(8 * i, 8), pl.ds((j - rel_cols) * LANES, LANES)] = o_ar[tile_place(t)]
    g = acc_rel[...]
    state = rel_state[...] + jnp.sum(g * g, axis=0, keepdims=True) * (1.0 / dims.dim)
    rel_state_out[...] = state
    rel_t_out[...] = rel_t[...] - LEARN_RATE * g / jnp.sqrt(state[:1] + ADA_EPS)
    for c in range(dims.negp // CHUNK):
        put_rows(neg_g, c, rows_of(acc_neg[:, pl.ds(c * CHUNK, CHUNK)]))
    if late:
        tail_gradients()

    neg_pair.wait_send()
    neg_pair2.wait_send()
    ar_pair.wait_send()
    ar_pair2.wait_send()
    if s:
        dp_copy.wait_send()

        loop(0, nch, lambda c: tail_copy(c).wait_send())
        for c in range(nch):
            if plan[2] == nch or c >= nch - AHEAD or c < plan[2] - AHEAD:
                head_copy(c).wait_send()

    if s == 0:
        def moved(k):
            rel_copy(k).wait()
        loop(1, dims.rounds, moved)
        for k in range(1, dims.rounds):
            id_copy(k).wait()

    def sent_peers(k):
        rs_neg(k).wait_send()
        ag_neg(k).wait_send()
        rs_ar(k).wait_send()
        ag_ar(k).wait_send()
    loop(1, chips, sent_peers)


def bucket_step(dims, s, rows_in, rel_t, rel_state, rel_ids, rel_ids_p, weight, extra):
    d = dims
    vm = pl.BlockSpec(memory_space=VMEM)
    sds = jax.ShapeDtypeStruct
    dma = pltpu.SemaphoreType.DMA
    outs = [sds((2 * d.edges, LANES), F32), sds((2 * d.edges, LANES), F32), sds((2 * d.negp, LANES), F32),
            sds((d.dc, d.relp), F32), sds((8, d.relp), F32), sds((8, CHUNK), F32)]
    if extra:
        outs += [sds(extra[1].shape, I32)] + [sds((d.edges,), I32)] * (d.rounds - 1)
    tail, head, neg = rows_in
    rows = VMEM((d.nch, d.dc, CHUNK), BF16)
    wide = VMEM((d.nch, d.dc, CHUNK), F32)
    line = VMEM((d.nch, CHUNK), F32)
    neg_part = VMEM((d.chips, d.negc, 2 * LANES), BF16)
    ar_part = VMEM((d.chips, d.tpd, 8, LANES), F32)
    scratch = [dma((2, d.rounds))] * 2 if extra else []
    scratch += [rows, rows, line, line,
                VMEM((3 * d.dc, d.relp), BF16), wide, wide, VMEM((d.nch, 2 * LANES, CHUNK), BF16),
                VMEM((d.nch, d.negp, CHUNK), F32), line, line,
                neg_part, neg_part, neg_part, VMEM((d.negc, 2 * LANES), BF16),
                VMEM((2, d.chips, d.negc, 2 * LANES), BF16), VMEM((2 * LANES, d.negp), BF16),
                VMEM((d.dc, d.relp), F32), VMEM((d.dc, d.negp), F32), wide,
                VMEM((2, d.chips, d.tpd, 8, LANES), F32), ar_part, ar_part, ar_part,
                VMEM((d.tpd, 8, LANES), F32), VMEM((2, d.chips, d.tpd, 8, LANES), F32),
                dma((d.nch,)), dma((d.nch,)), dma((d.nch,)), dma((d.nch,)), dma((5,)), dma((5,))]
    scratch += [dma((d.chips,))] * 8
    return pl.pallas_call(
        functools.partial(bucket_kernel, d, s), out_shape=outs,
        in_specs=[vm] * (8 + len(extra)), out_specs=[vm] * len(outs),
        scratch_shapes=scratch, name=f'bucket_{s}',
        compiler_params=pltpu.CompilerParams(collective_id=s, has_side_effects=True, vmem_limit_bytes=36 << 20),
    )(head, tail, neg.reshape(2, d.chips, d.negc, 2 * LANES), rel_t, rel_state, rel_ids, rel_ids_p, weight, *extra)


def solution(mesh):
    row_spec = P(('sweep', 'ent'), None)
    flat_spec = P(('sweep', 'ent'))
    rel_spec = P('sweep', None)
    state_spec = P('sweep')
    edge_spec = P(('sweep', 'ent'), None, None)

    def device_fn(ent_emb, ent_ada, rel_emb, rel_ada, head_idx, tail_idx, rel_idx, edge_mask, neg_idx):
        d = Dims(mesh, ent_emb, rel_emb, head_idx, neg_idx)
        me = lax.axis_index('ent')
        table = pack(d, ent_emb, ent_ada)
        rel = jnp.pad(rel_emb.reshape(d.num_rel, 2, d.half), ((0, d.relp - d.num_rel), (0, 0), (0, d.hp - d.half)))
        rel_t = rel.reshape(d.relp, d.dc).T
        rel_state = jnp.broadcast_to(jnp.pad(rel_ada, (0, d.relp - d.num_rel), constant_values=1.0), (8, d.relp))

        head_ids = (head_idx[0] * 2).reshape(-1)
        own_tail_ids = (tail_idx[0] * 2).reshape(-1)
        local = neg_idx - me * d.rows
        owned = (local >= 0) & (local < d.rows)
        neg_all = jnp.pad(jnp.where(owned, local, d.rows) * 2, ((0, 0), (0, d.negp - d.neg)), constant_values=2 * d.rows)
        place = lax.broadcasted_iota(I32, neg_all.shape, 1)
        key = jnp.where(neg_all < 2 * d.rows, place, place + d.negp)
        key, neg_rows = lax.sort((key, neg_all), dimension=1, num_keys=1)
        neg_src = key % d.negp * 2
        counts = jnp.sum(owned.astype(I32), axis=1)
        rel_ids = rel_idx[0].reshape(d.rounds * d.nch, CHUNK)
        weight = edge_mask[0].astype(F32).reshape(d.rounds * d.nch, CHUNK)
        def per_round(x):
            size = x.size // d.rounds
            return [x.reshape(-1)[k * size:(k + 1) * size] for k in range(d.rounds)]
        heads, counts, neg_rows, neg_src = (per_round(x) for x in (head_ids, counts, neg_rows, neg_src))
        first_tails = own_tail_ids[:d.edges]
        table, heads, counts, neg_rows, neg_src, first_tails = lax.optimization_barrier((table, heads, counts, neg_rows, neg_src, first_tails))

        def lists(k):
            return [counts[k], heads[k], tails[k], neg_rows[k], neg_src[k]]
        tails = [first_tails]
        rows_in = table_step(d, None, lists(0), None, table)
        losses = []
        for s in range(d.rounds):
            if s == 0:
                res = bucket_step(d, s, rows_in, rel_t, rel_state, rel_ids, rel_ids, weight, (own_tail_ids, rel_ids))
                rel_ids_p = res[6]
                tails += res[7:]
            else:
                res = bucket_step(d, s, rows_in, rel_t, rel_state, rel_ids, rel_ids_p, weight, ())
            hg, tg, ng, rel_t, rel_state, loss = res[:6]
            losses.append(loss)
            table, *rows_in = table_step(d, lists(s), lists(s + 1) if s + 1 < d.rounds else None, (hg, tg, ng), table)
        loss = jnp.sum(jnp.stack(losses), axis=(1, 2)) / d.edges
        emb, ada = unpack(d, table)
        rel_out = rel_t.T.reshape(d.relp, 2, d.hp)[:d.num_rel, :, :d.half].reshape(d.num_rel, d.dim)
        return emb, ada, rel_out, rel_state[0, :d.num_rel], loss[None, :]

    return jax.shard_map(device_fn, mesh=mesh,
                         in_specs=(row_spec, flat_spec, rel_spec, state_spec, edge_spec, edge_spec, edge_spec, edge_spec, rel_spec),
                         out_specs=(row_spec, flat_spec, rel_spec, state_spec, row_spec), check_vma=False)
```

```python
import functools

import jax
import jax.numpy as jnp
from jax import lax
from jax.experimental import pallas as pl
from jax.experimental.pallas import tpu as pltpu
from jax.sharding import PartitionSpec as P

LEARN_RATE = 0.05
ADA_EPS = 1e-10
LANES = 128
CHUNK = 256
PACK_ROWS = 1024
QUERY_GROUP, SCORE_GROUP, HEAD_GROUP, ROWS_GROUP, TAIL_GROUP = 2, 2, 2, 4, 2
TAILS_FIRST, TAILS_SECOND = 0, 2
AHEAD = 2
HEAD_SENDS = {0: (0, 2, 3, 4, 5, 7, 8), **{k: (2, 8, 8, 8, 8, 8, 8) for k in (1, 2, 3, 6, 7, 8)}}
F32, BF16, I32 = jnp.float32, jnp.bfloat16, jnp.int32
MESH = pl.DeviceIdType.MESH
VMEM = pltpu.VMEM


def round_up(value, multiple):
    return -(-value // multiple) * multiple


class Dims:
    def __init__(self, mesh, ent_emb, rel_emb, head_idx, neg_idx):
        self.ent = mesh.shape['ent']
        self.chips = self.ent // 2
        self.rows, self.dim = ent_emb.shape
        self.half = self.dim // 2
        self.hp = round_up(self.half, 8)
        self.dc = 2 * self.hp
        self.num_rel = rel_emb.shape[0]
        self.relp = round_up(self.num_rel, LANES)
        self.rounds, self.edges = head_idx.shape[1:]
        self.nch = self.edges // CHUNK
        self.neg = neg_idx.shape[1]
        self.negp = round_up(self.neg, self.ent * 16)
        self.negc = self.negp // self.ent
        self.cols = (self.relp + self.negp) // LANES
        self.tiles = self.dc // 8 * self.cols
        self.tpd = -(-self.tiles // self.ent)
        self.trows = 2 * self.rows + 16


def nt_dot(lhs, rhs):
    return lax.dot_general(lhs, rhs, (((1,), (1,)), ((), ())), preferred_element_type=F32)


def nn_dot(lhs, rhs):
    return jnp.dot(lhs, rhs, preferred_element_type=F32)


def split3(x):
    hi = x.astype(BF16)
    rest = x - hi.astype(F32)
    mid = rest.astype(BF16)
    lo = (rest - mid.astype(F32)).astype(BF16)
    return hi, mid, lo


def iota(shape, dim):
    return lax.broadcasted_iota(I32, shape, dim)


def eye(n):
    return jnp.where(iota((n, n), 0) == iota((n, n), 1), 1.0, 0.0).astype(BF16)


def compact_sel(dims, out_rows):
    c = iota((out_rows, 2 * LANES), 0)
    lane = iota((out_rows, 2 * LANES), 1)
    src = jnp.where(c < dims.hp, c, c - dims.hp + LANES)
    return jnp.where((lane == src) & (c < dims.dc), 1.0, 0.0).astype(BF16)


def pack_kernel(half, last, e_ref, g_ref, o_ref):
    step = pl.program_id(0)
    row = iota((LANES, LANES), 0)
    low = half // 8 * 8
    gap = jnp.zeros((LANES - round_up(half, 8), LANES), F32)

    @pl.when(step < last)
    def _():
        for i in range(PACK_ROWS // LANES):
            cols = pl.ds(i * LANES, LANES)
            re = jnp.concatenate([e_ref[pl.ds(0, round_up(half, 8)), cols], gap], axis=0)
            re = jnp.where(row < half, re, 0.0)
            im = jnp.concatenate([e_ref[pl.ds(low, 2 * half - low), cols], jnp.zeros((LANES - (2 * half - low), LANES), F32)], axis=0)
            if half > low:
                im = pltpu.roll(im, LANES - (half - low), 0)
            im = jnp.where(row < half, im, 0.0)
            im = jnp.where(row == LANES - 1, g_ref[pl.ds(i, 1), :], im)
            o_ref[pl.ds(2 * i * LANES, LANES, stride=2), :] = jnp.transpose(re)
            o_ref[pl.ds(2 * i * LANES + 1, LANES, stride=2), :] = jnp.transpose(im)

    @pl.when(step == last)
    def _():
        o_ref[...] = jnp.zeros_like(o_ref)


def pack(dims, emb, ada):
    blocks = dims.rows // PACK_ROWS
    return pl.pallas_call(
        functools.partial(pack_kernel, dims.half, blocks),
        grid=(blocks + 1,),
        out_shape=jax.ShapeDtypeStruct((dims.trows, LANES), F32),
        in_specs=[pl.BlockSpec((dims.dim, PACK_ROWS), lambda i: (0, jnp.minimum(i, blocks - 1))),
                  pl.BlockSpec((PACK_ROWS // LANES, LANES), lambda i: (jnp.minimum(i, blocks - 1), 0))],
        out_specs=pl.BlockSpec((2 * PACK_ROWS, LANES), lambda i: (i, 0)),
        compiler_params=pltpu.CompilerParams(vmem_limit_bytes=16 << 20),
        name='pack')(emb.T, ada.reshape(dims.rows // LANES, LANES))


def unpack_kernel(half, t_ref, e_ref, g_ref):
    low = half // 8 * 8
    high = round_up(half, 8)
    for i in range(PACK_ROWS // LANES):
        cols = pl.ds(i * LANES, LANES)
        re = jnp.transpose(t_ref[pl.ds(2 * i * LANES, LANES, stride=2), :])
        im = jnp.transpose(t_ref[pl.ds(2 * i * LANES + 1, LANES, stride=2), :])
        g_ref[pl.ds(i, 1), :] = im[LANES - 1:]
        e_ref[pl.ds(0, low), cols] = re[:low]
        if half > low:
            im = pltpu.roll(im, half - low, 0)
            e_ref[pl.ds(low, 8), cols] = jnp.where(iota((8, LANES), 0) < half - low, re[low:high], im[:8])
            e_ref[pl.ds(high, 2 * half - high), cols] = im[8:8 + 2 * half - high]
        else:
            e_ref[pl.ds(half, half), cols] = im[:half]


def unpack(dims, table):
    blocks = dims.rows // PACK_ROWS
    emb, ada = pl.pallas_call(
        functools.partial(unpack_kernel, dims.half),
        grid=(blocks,),
        out_shape=[jax.ShapeDtypeStruct((dims.dim, dims.rows), F32),
                   jax.ShapeDtypeStruct((dims.rows // LANES, LANES), F32)],
        in_specs=[pl.BlockSpec((2 * PACK_ROWS, LANES), lambda i: (i, 0))],
        out_specs=[pl.BlockSpec((dims.dim, PACK_ROWS), lambda i: (0, i)),
                   pl.BlockSpec((PACK_ROWS // LANES, LANES), lambda i: (i, 0))],
        compiler_params=pltpu.CompilerParams(vmem_limit_bytes=16 << 20),
        name='unpack')(table)
    return emb.T, ada.reshape(dims.rows)


UNROLL_SCATTER = 16
UNROLL_GATHER = 64
UNROLL_NEG = 8
CONVERT_GROUP = 4
UPDATE_ROWS = 512


def table_kernel(dims, old, new, *refs):
    refs = list(refs)
    update_rows, gather_next = old is not None, new is not None

    def take(n):
        taken = refs[:n]
        del refs[:n]
        return taken
    edges, negp = dims.edges, dims.negp
    sources, lists = [], []
    if update_rows:
        old_count, = take(1)
        sources += take(4)
    if gather_next:
        new_count, = take(1)
        sources += take(4)
    if update_rows:
        head_g, tail_g, neg_g = take(3)
    table_in, = take(1)
    table, = take(1) if update_rows else (table_in,)
    if gather_next:
        tail_out, head_out, neg_out = take(3)
    lists = take(len(sources))
    sem, = take(1)
    if update_rows:
        acc_a, acc_b = take(2)
    steps = [old] * 4 * (old is not None) + [new] * 4 * (new is not None)
    copies = [pltpu.make_async_copy(src.at[pl.ds(step * dst.shape[0], dst.shape[0])], dst, sem.at[k])
              for k, (src, dst, step) in enumerate(zip(sources, lists, steps))]
    for copy in copies:
        copy.start()
    if update_rows:
        head_i, tail_i, neg_i, src_i = lists[:4]
        table_update(dims, copies, old_count[old], head_i, tail_i, neg_i, src_i, head_g, tail_g, neg_g, table_in, table, acc_a, acc_b)
    else:
        for copy in copies:
            copy.wait()
    if gather_next:
        head_i, tail_i, neg_i, src_i = lists[-4:]
        for ids, out in ((tail_i, tail_out), (head_i, head_out)):
            def gather(c, _):
                for u in range(UNROLL_GATHER):
                    k = c * UNROLL_GATHER + u
                    out[pair(k), :] = table[at(ids, k), :]
                return 0
            lax.fori_loop(0, edges // UNROLL_GATHER, gather, 0)

        neg_out[...] = jnp.zeros_like(neg_out)

        def gather_neg(c, _):
            rows = [table[at(neg_i, c * UNROLL_NEG + u), :] for u in range(UNROLL_NEG)]
            for u in range(UNROLL_NEG):
                neg_out[at(src_i, c * UNROLL_NEG + u), :] = rows[u]
            return 0
        lax.fori_loop(0, (new_count[new] + UNROLL_NEG - 1) // UNROLL_NEG, gather_neg, 0)


def table_update(dims, copies, count, head_i, tail_i, neg_i, src_i, head_g, tail_g, neg_g, table_in, table, acc_a, acc_b):
    edges = dims.edges

    def zero(c, _):
        rows = pl.ds(pl.multiple_of(c * 256, 256), 256)
        acc_a[rows, :] = jnp.zeros((256, LANES), F32)
        acc_b[rows, :] = jnp.zeros((256, LANES), F32)
        return 0
    lax.fori_loop(0, 2 * dims.rows // 256, zero, 0)
    for copy in copies:
        copy.wait()

    def scatter(c, _):
        for u in range(0, UNROLL_SCATTER, 2):
            k = c * UNROLL_SCATTER + u
            h0, h1, t0, t1 = at(head_i, k), at(head_i, k + 1), at(tail_i, k), at(tail_i, k + 1)
            a0 = acc_a[h0, :] + head_g[pair(k), :]
            b0 = acc_b[t0, :] + tail_g[pair(k), :]
            a1 = jnp.where(head_i[k] == head_i[k + 1], a0, acc_a[h1, :]) + head_g[pair(k + 1), :]
            b1 = jnp.where(tail_i[k] == tail_i[k + 1], b0, acc_b[t1, :]) + tail_g[pair(k + 1), :]
            acc_a[h0, :] = a0
            acc_b[t0, :] = b0
            acc_a[h1, :] = a1
            acc_b[t1, :] = b1
        return 0
    lax.fori_loop(0, edges // UNROLL_SCATTER, scatter, 0)

    def scatter_neg(c, _):
        for u in range(0, UNROLL_NEG, 2):
            k = c * UNROLL_NEG + u
            h, t = at(neg_i, k), at(neg_i, k + 1)
            new_a = acc_a[h, :] + neg_g[at(src_i, k), :]
            new_b = acc_b[t, :] + neg_g[at(src_i, k + 1), :]
            acc_a[h, :] = new_a
            acc_b[t, :] = new_b
        return 0
    lax.fori_loop(0, (count + UNROLL_NEG - 1) // UNROLL_NEG, scatter_neg, 0)

    lane = iota((UPDATE_ROWS, LANES), 1)

    def update(c, _):
        base = pl.multiple_of(c * 2 * UPDATE_ROWS, 2 * UPDATE_ROWS)
        re = pl.ds(base, UPDATE_ROWS, stride=2)
        im = pl.ds(base + 1, UPDATE_ROWS, stride=2)
        g_re = acc_a[re, :] + acc_b[re, :]
        g_im = acc_a[im, :] + acc_b[im, :]
        e_re, e_im = table_in[re, :], table_in[im, :]
        part = (g_re * g_re + g_im * g_im) * (1.0 / dims.dim)
        part = jnp.where(lane == LANES - 1, e_im, part)
        state = jnp.sum(part, axis=1, keepdims=True)
        rate = LEARN_RATE * lax.rsqrt(state + ADA_EPS)
        table[re, :] = e_re - rate * g_re
        table[im, :] = jnp.where(lane == LANES - 1, state, e_im - rate * g_im)
        return 0
    lax.fori_loop(0, dims.rows // UPDATE_ROWS, update, 0)
    table[pl.ds(2 * dims.rows, 16), :] = jnp.zeros((16, LANES), F32)


def pair(k):
    return pl.ds(pl.multiple_of(2 * k, 2), 2)


def at(ref, k):
    return pl.ds(pl.multiple_of(ref[k], 2), 2)


def table_step(dims, old, new, old_lists, new_lists, grads, table):
    vm = pl.BlockSpec(memory_space=VMEM)
    smem = pl.BlockSpec(memory_space=pltpu.SMEM)
    anys = pl.BlockSpec(memory_space=pl.ANY)
    sizes = (dims.edges, dims.edges, dims.negp, dims.negp)
    operands, in_specs, outs, scratch, aliases = [], [], [], [], {}
    for step, lists in ((old, old_lists), (new, new_lists)):
        if step is not None:
            operands += lists
            in_specs += [smem] + [anys] * 4
            scratch += [pltpu.SMEM((n,), I32) for n in sizes]
    scratch.append(pltpu.SemaphoreType.DMA((len(scratch),)))
    if old is not None:
        operands += grads
        in_specs += [vm] * 3
        aliases = {len(operands): 0}
        outs.append(jax.ShapeDtypeStruct((dims.trows, LANES), F32))
        scratch += [VMEM((dims.trows, LANES), F32)] * 2
    operands.append(table)
    in_specs.append(vm)
    if new is not None:
        outs += [jax.ShapeDtypeStruct((2 * n, LANES), F32) for n in (dims.edges, dims.edges, dims.negp)]
    return pl.pallas_call(
        functools.partial(table_kernel, dims, old, new),
        out_shape=outs, in_specs=in_specs, out_specs=[vm] * len(outs), scratch_shapes=scratch,
        input_output_aliases=aliases, name='table',
        compiler_params=pltpu.CompilerParams(vmem_limit_bytes=24 << 20))(*operands)


def bucket_kernel(dims, s, *refs):
    (head_rows_in, tail_rows_in, neg_rows_in, rel_t, rel_state, rel_ids, rel_ids_p, weight), refs = refs[:8], refs[8:]
    if s == 0:
        (tail_x, rel_x), refs = refs[:2], refs[2:]
    (head_g, tail_g, neg_g, rel_t_out, rel_state_out, loss), refs = refs[:6], refs[6:]
    if s == 0:
        (rel_x_out, tail_x_out), refs = refs[:2], refs[2:]
        (x_ss, x_rs), refs = refs[:2], refs[2:]
    (head, tail, neg, tail_r, head_r, dp_s, dp_r, splits, q_all, r_all, qb, ex, top_s, sum_s, neg_p, neg_half, neg_buf, neg_acc, neg_all, neg_t,
     acc_rel, acc_neg, head_c, x_ar, p_ar, half_ar, buf_ar, acc_ar, o_ar,
     tail_ss, tail_rs, head_ss, head_rs, one_s, one_r, rs_s, rs_r, ag_s, ag_r, rs2_s, rs2_r, ag2_s, ag2_r) = refs
    ent, chips, hp, dc, nch = dims.ent, dims.chips, dims.hp, dims.dc, dims.nch
    me = lax.axis_index('ent')
    core, chip = lax.rem(me, 2), me // 2
    partner = me + 1 - 2 * core
    dst_t = lax.rem(me + ent - s, ent)
    dst_h = lax.rem(me + s, ent)

    def dev(d):
        return {'ent': d}

    def peer(k):
        return lax.rem(chip + k, chips) * 2 + core

    def remote(src, dst, ss, rs, d):
        return pltpu.make_async_remote_copy(src_ref=src, dst_ref=dst, send_sem=ss, recv_sem=rs, device_id=dev(d), device_id_type=MESH)

    def loop(lo, hi, fn):
        def body(k, _):
            fn(k)
            return 0
        lax.fori_loop(lo, hi, body, 0)

    def chunks(group, fn):
        loop(0, nch // group, lambda k: fn([k * group + i for i in range(group)]))

    barrier = pltpu.get_barrier_semaphore()

    def signal(d):
        pl.semaphore_signal(barrier, inc=1, device_id=dev(d), device_id_type=MESH)
    if s:
        signal(dst_t)
        signal(dst_h)
        others = 2
    else:
        loop(1, dims.rounds, lambda k: signal(lax.rem(me + ent - k, ent)))
        others = dims.rounds - 1
    loop(1, chips, lambda k: signal(peer(k)))
    signal(partner)

    def one_hot(ids_ref, c):
        ids = ids_ref[pl.ds(s * nch + c, 1), :]
        return jnp.where(iota((dims.relp, CHUNK), 0) == ids, 1.0, 0.0).astype(BF16)

    def rel_rows(hot):
        r = nn_dot(splits[...], hot)
        return (r[:dc] + r[dc:2 * dc]) + r[2 * dc:]

    def queries(rows, r):
        x = rows.astype(F32)
        h_re, h_im, r_re, r_im = x[:hp], x[hp:], r[:hp], r[hp:]
        return jnp.concatenate([h_re * r_re - h_im * r_im, h_re * r_im + h_im * r_re], axis=0)

    def rel_query(cs):
        for c in cs:
            r_all[c] = rel_rows(one_hot(rel_ids, c))

    def head_query(cs):
        for c in cs:
            q = queries(head[c], r_all[c])
            q_all[c] = q
            qb[c, pl.ds(0, dc), :] = q.astype(BF16)

    ident = eye(CHUNK)
    for c in range(nch):
        qb[c, pl.ds(dc, 2 * LANES - dc), :] = jnp.zeros((2 * LANES - dc, CHUNK), BF16)
    acc_rel[...] = jnp.zeros_like(acc_rel)
    acc_neg[...] = jnp.zeros_like(acc_neg)
    loss[...] = jnp.zeros_like(loss)
    sel = compact_sel(dims, 2 * LANES)

    def edge_rows(ref, c):
        base = pl.multiple_of(c * 2 * CHUNK, 2 * CHUNK)
        re = ref[pl.ds(base, CHUNK, stride=2), :]
        im = ref[pl.ds(base + 1, CHUNK, stride=2), :]
        return jnp.concatenate([re.astype(BF16), im.astype(BF16)], axis=1)

    def convert(ref, out):
        def group(cs):
            for c in cs:
                out[c] = nt_dot(sel[:dc], edge_rows(ref, c)).astype(BF16)
        chunks(CONVERT_GROUP, group)
    per = CHUNK // dims.negc
    for c in range(dims.negp // CHUNK):
        neg[c * per // chips, pl.ds(c * per % chips, per)] = nt_dot(edge_rows(neg_rows_in, c), sel).astype(BF16).reshape(per, dims.negc, 2 * LANES)
    convert(tail_rows_in, tail)

    pl.semaphore_wait(barrier, chips + others)

    def tail_copy(c):
        return remote(tail.at[c], tail_r.at[c], tail_ss.at[c], tail_rs.at[c], dst_t)

    def head_copy(c):
        return remote(head.at[c], head_r.at[c], head_ss.at[c], head_rs.at[c], dst_h)

    def send_tails(lo, hi):
        if s:
            loop(lo, hi, lambda c: tail_copy(c).start())

    def send_heads(lo, hi):
        if s and hi > lo:
            loop(lo, hi, lambda c: head_copy(c).start())
    plan = (0,) + HEAD_SENDS.get(s, HEAD_SENDS[0])
    late = s > 0 and plan[2] < nch

    def send_heads_at(point):
        if point < 2:
            send_heads(plan[point], plan[point + 1])
        elif s:
            for c in range(plan[point], plan[point + 1]):
                if c >= AHEAD:
                    head_copy(c - AHEAD).wait_send()
                head_copy(c).start()
    if s:
        tail_in, head_in, dp_in = tail_r, head_r, dp_r
    else:
        tail_in, head_in, dp_in = tail, head, dp_s

    send_tails(0, TAILS_FIRST)
    neg_pair = remote(neg.at[1 - core], neg_p, one_s.at[0], one_r.at[0], partner)
    neg_pair.start()
    neg_pair.wait_recv()
    neg_half[...] = neg[core] + neg_p[...]

    def rs_neg(k):
        return remote(neg_half.at[lax.rem(chip + k, chips)], neg_buf.at[k], rs_s.at[k], rs_r.at[k], peer(k))
    loop(1, chips, lambda k: rs_neg(k).start())
    send_tails(TAILS_FIRST, TAILS_SECOND)
    convert(head_rows_in, head)
    send_heads_at(0)
    neg_acc[...] = neg_half[chip]

    def take_neg(k):
        rs_neg(k).wait_recv()
        neg_acc[...] = neg_acc[...] + neg_buf[k]
    loop(1, chips, take_neg)

    def ag_neg(k):
        return remote(neg_acc, neg_all.at[core, chip], ag_s.at[k], ag_r.at[k], peer(k))
    loop(1, chips, lambda k: ag_neg(k).start())
    send_tails(TAILS_SECOND, nch)
    send_heads_at(1)
    if s == 0:
        def rel_copy(k):
            rows = pl.ds(pl.multiple_of(k * nch, nch), nch)
            return remote(rel_x.at[rows], rel_x_out.at[rows], x_ss.at[0, k], x_rs.at[0, k], lax.rem(me + k, ent))

        def id_copy(k):
            rows = pl.ds(k * dims.edges, dims.edges)
            return remote(tail_x.at[rows], tail_x_out.at[rows], x_ss.at[1, k], x_rs.at[1, k], lax.rem(me + k, ent))
        loop(1, dims.rounds, lambda k: rel_copy(k).start())
        for k in range(1, dims.rounds):
            id_copy(k).start()
        rel_x_out[pl.ds(0, nch), :] = rel_x[pl.ds(0, nch), :]
        tail_x_out[pl.ds(0, dims.edges)] = tail_x[pl.ds(0, dims.edges)]
    for i, part in enumerate(split3(rel_t[...])):
        splits[pl.ds(i * dc, dc), :] = part
    chunks(QUERY_GROUP, rel_query)
    chunks(QUERY_GROUP, head_query)
    neg_all[core, chip] = neg_acc[...]
    loop(1, chips, lambda k: ag_neg(k).wait_recv())
    neg_pair2 = remote(neg_all.at[core], neg_all.at[core], one_s.at[1], one_r.at[1], partner)
    neg_pair2.start()
    neg_pair2.wait_recv()
    neg_t[...] = nt_dot(eye(2 * LANES), neg_all[...].reshape(dims.negp, 2 * LANES)).astype(BF16)

    main = dims.neg // 16 * 16

    def score(cs):
        for c in cs:
            scores = nn_dot(neg_all[...].reshape(dims.negp, 2 * LANES), qb[c])
            body = scores[:main]
            top = jnp.max(body, axis=0, keepdims=True)
            if main < dims.negp:
                rest = jnp.where(iota((dims.negp - main, CHUNK), 0) < dims.neg - main, scores[main:], -1e30)
                top = jnp.maximum(top, jnp.max(rest, axis=0, keepdims=True))
            e_body = jnp.exp(body - top)
            ex[c, pl.ds(0, main), :] = e_body
            total = jnp.sum(e_body, axis=0, keepdims=True)
            if main < dims.negp:
                e_rest = jnp.exp(rest - top)
                ex[c, pl.ds(main, dims.negp - main), :] = e_rest
                total = total + jnp.sum(e_rest, axis=0, keepdims=True)
            top_s[pl.ds(c, 1), :] = top
            sum_s[pl.ds(c, 1), :] = total
    chunks(SCORE_GROUP, score)

    def head_side(cs):
        if s:
            for c in cs:
                tail_copy(c).wait_recv()
        lost, neg_q, neg_d, rel_parts, rel_hot = [], [], [], [], []
        for c in cs:
            t = tail_in[c].astype(F32)
            pos = jnp.sum(q_all[c] * t, axis=0, keepdims=True)
            neg_top = top_s[pl.ds(c, 1), :]
            top = jnp.maximum(pos, neg_top)
            pos_exp = jnp.exp(pos - top)
            scale = jnp.exp(neg_top - top)
            norm = pos_exp + scale * sum_s[pl.ds(c, 1), :]
            w = weight[pl.ds(s * nch + c, 1), :]
            lost.append(w * (top + jnp.log(norm) - pos))
            dp = w * (pos_exp / norm - 1.0)
            dp_s[pl.ds(c, 1), :] = dp
            ds = (ex[c] * (w * scale / norm)).astype(BF16)
            g = dp * t + nn_dot(neg_t[pl.ds(0, dc), :], ds)
            neg_q.append(qb[c, pl.ds(0, dc), :])
            neg_d.append(ds)
            g_re, g_im = g[:hp], g[hp:]
            r = r_all[c]
            r_re, r_im = r[:hp], r[hp:]
            head_c[c] = jnp.concatenate([g_re * r_re + g_im * r_im, g_im * r_re - g_re * r_im], axis=0)
            h = head[c].astype(F32)
            h_re, h_im = h[:hp], h[hp:]
            rel_g = jnp.concatenate([g_re * h_re + g_im * h_im, g_im * h_re - g_re * h_im], axis=0)
            rel_parts.append(jnp.concatenate(split3(rel_g), axis=0))
            rel_hot.append(one_hot(rel_ids, c))
        loss[pl.ds(0, 1), :] += sum(lost)
        acc_neg[...] += nt_dot(jnp.concatenate(neg_q, axis=1), jnp.concatenate(neg_d, axis=1))
        part = nt_dot(jnp.concatenate(rel_parts, axis=1), jnp.concatenate(rel_hot, axis=1))
        acc_rel[...] += (part[:dc] + part[dc:2 * dc]) + part[2 * dc:]
    chunks(HEAD_GROUP, head_side)

    if s:
        dp_copy = remote(dp_s, dp_r, one_s.at[2], one_r.at[2], dst_h)
        dp_copy.start()

    def tile_place(t):
        d, j = t // dims.tpd, t % dims.tpd
        return d // chips, d % chips, j
    rel_cols = dims.relp // LANES
    for t in range(dims.tpd * ent):
        i, j = t // dims.cols, t % dims.cols
        if t >= dims.tiles:
            x_ar[tile_place(t)] = jnp.zeros((8, LANES), F32)
        elif j < rel_cols:
            x_ar[tile_place(t)] = acc_rel[pl.ds(8 * i, 8), pl.ds(j * LANES, LANES)]
        else:
            x_ar[tile_place(t)] = acc_neg[pl.ds(8 * i, 8), pl.ds((j - rel_cols) * LANES, LANES)]

    ar_pair = remote(x_ar.at[1 - core], p_ar, one_s.at[3], one_r.at[3], partner)
    ar_pair.start()
    send_heads_at(2)

    def rows_of(cols):
        gap = jnp.zeros((LANES - hp, CHUNK), F32)
        x = jnp.concatenate([cols[:hp], gap, cols[hp:], gap], axis=0)
        return nt_dot(jnp.concatenate([ident] * 3, axis=1), jnp.concatenate(split3(x), axis=1))

    def put_rows(out, c, rows):
        base = pl.multiple_of(c * 2 * CHUNK, 2 * CHUNK)
        out[pl.ds(base, CHUNK, stride=2), :] = rows[:, :LANES]
        out[pl.ds(base + 1, CHUNK, stride=2), :] = rows[:, LANES:]

    def head_rows(cs):
        for c in cs:
            put_rows(head_g, c, rows_of(head_c[c]))

    def tail_side(cs):
        if s:
            for c in cs:
                head_copy(c).wait_recv()
        for c in cs:
            q = queries(head_in[c], rel_rows(one_hot(rel_ids_p, c)))
            put_rows(tail_g, c, rows_of(dp_in[pl.ds(c, 1), :] * q))

    ar_pair.wait_recv()
    half_ar[...] = x_ar[core] + p_ar[...]

    def rs_ar(k):
        return remote(half_ar.at[lax.rem(chip + k, chips)], buf_ar.at[k], rs2_s.at[k], rs2_r.at[k], peer(k))
    loop(1, chips, lambda k: rs_ar(k).start())
    send_heads_at(3)
    chunks(ROWS_GROUP, head_rows)
    send_heads_at(4)
    acc_ar[...] = half_ar[chip]

    def take_ar(k):
        rs_ar(k).wait_recv()
        acc_ar[...] += buf_ar[k]
    loop(1, chips, take_ar)

    def ag_ar(k):
        return remote(acc_ar, o_ar.at[core, chip], ag2_s.at[k], ag2_r.at[k], peer(k))
    loop(1, chips, lambda k: ag_ar(k).start())
    send_heads_at(5)
    o_ar[core, chip] = acc_ar[...]
    def tail_gradients():
        if s:
            dp_copy.wait_recv()
        chunks(TAIL_GROUP, tail_side)
    if not late:
        tail_gradients()
    loop(1, chips, lambda k: ag_ar(k).wait_recv())
    ar_pair2 = remote(o_ar.at[core], o_ar.at[core], one_s.at[4], one_r.at[4], partner)
    ar_pair2.start()
    send_heads_at(6)
    ar_pair2.wait_recv()

    for t in range(dims.tiles):
        i, j = t // dims.cols, t % dims.cols
        if j < rel_cols:
            acc_rel[pl.ds(8 * i, 8), pl.ds(j * LANES, LANES)] = o_ar[tile_place(t)]
        else:
            acc_neg[pl.ds(8 * i, 8), pl.ds((j - rel_cols) * LANES, LANES)] = o_ar[tile_place(t)]
    g = acc_rel[...]
    state = rel_state[...] + jnp.sum(g * g, axis=0, keepdims=True) * (1.0 / dims.dim)
    rel_state_out[...] = state
    rel_t_out[...] = rel_t[...] - LEARN_RATE * g / jnp.sqrt(state[:1] + ADA_EPS)
    for c in range(dims.negp // CHUNK):
        put_rows(neg_g, c, rows_of(acc_neg[:, pl.ds(c * CHUNK, CHUNK)]))
    if late:
        tail_gradients()

    neg_pair.wait_send()
    neg_pair2.wait_send()
    ar_pair.wait_send()
    ar_pair2.wait_send()
    if s:
        dp_copy.wait_send()

        loop(0, nch, lambda c: tail_copy(c).wait_send())
        for c in range(nch):
            if plan[2] == nch or c >= nch - AHEAD or c < plan[2] - AHEAD:
                head_copy(c).wait_send()

    if s == 0:
        def moved(k):
            rel_copy(k).wait()
        loop(1, dims.rounds, moved)
        for k in range(1, dims.rounds):
            id_copy(k).wait()

    def sent_peers(k):
        rs_neg(k).wait_send()
        ag_neg(k).wait_send()
        rs_ar(k).wait_send()
        ag_ar(k).wait_send()
    loop(1, chips, sent_peers)


def bucket_step(dims, s, rows_in, rel_t, rel_state, rel_ids, rel_ids_p, weight, extra):
    d = dims
    vm = pl.BlockSpec(memory_space=VMEM)
    sds = jax.ShapeDtypeStruct
    dma = pltpu.SemaphoreType.DMA
    outs = [sds((2 * d.edges, LANES), F32), sds((2 * d.edges, LANES), F32), sds((2 * d.negp, LANES), F32),
            sds((d.dc, d.relp), F32), sds((8, d.relp), F32), sds((8, CHUNK), F32)]
    if extra:
        outs += [sds(extra[1].shape, I32), sds(extra[0].shape, I32)]
    tail, head, neg = rows_in
    rows = VMEM((d.nch, d.dc, CHUNK), BF16)
    wide = VMEM((d.nch, d.dc, CHUNK), F32)
    line = VMEM((d.nch, CHUNK), F32)
    neg_part = VMEM((d.chips, d.negc, 2 * LANES), BF16)
    ar_part = VMEM((d.chips, d.tpd, 8, LANES), F32)
    scratch = [dma((2, d.rounds))] * 2 if extra else []
    scratch += [rows, rows, VMEM((2, d.chips, d.negc, 2 * LANES), BF16), rows, rows, line, line,
                VMEM((3 * d.dc, d.relp), BF16), wide, wide, VMEM((d.nch, 2 * LANES, CHUNK), BF16),
                VMEM((d.nch, d.negp, CHUNK), F32), line, line,
                neg_part, neg_part, neg_part, VMEM((d.negc, 2 * LANES), BF16),
                VMEM((2, d.chips, d.negc, 2 * LANES), BF16), VMEM((2 * LANES, d.negp), BF16),
                VMEM((d.dc, d.relp), F32), VMEM((d.dc, d.negp), F32), wide,
                VMEM((2, d.chips, d.tpd, 8, LANES), F32), ar_part, ar_part, ar_part,
                VMEM((d.tpd, 8, LANES), F32), VMEM((2, d.chips, d.tpd, 8, LANES), F32),
                dma((d.nch,)), dma((d.nch,)), dma((d.nch,)), dma((d.nch,)), dma((5,)), dma((5,))]
    scratch += [dma((d.chips,))] * 8
    return pl.pallas_call(
        functools.partial(bucket_kernel, d, s), out_shape=outs,
        in_specs=[vm] * (8 + len(extra)), out_specs=[vm] * len(outs),
        scratch_shapes=scratch, name=f'bucket_{s}',
        compiler_params=pltpu.CompilerParams(collective_id=s, has_side_effects=True, vmem_limit_bytes=36 << 20),
    )(head, tail, neg, rel_t, rel_state, rel_ids, rel_ids_p, weight, *extra)


def solution(mesh):
    row_spec = P(('sweep', 'ent'), None)
    flat_spec = P(('sweep', 'ent'))
    rel_spec = P('sweep', None)
    state_spec = P('sweep')
    edge_spec = P(('sweep', 'ent'), None, None)

    def device_fn(ent_emb, ent_ada, rel_emb, rel_ada, head_idx, tail_idx, rel_idx, edge_mask, neg_idx):
        d = Dims(mesh, ent_emb, rel_emb, head_idx, neg_idx)
        me = lax.axis_index('ent')
        table = pack(d, ent_emb, ent_ada)
        rel = jnp.pad(rel_emb.reshape(d.num_rel, 2, d.half), ((0, d.relp - d.num_rel), (0, 0), (0, d.hp - d.half)))
        rel_t = rel.reshape(d.relp, d.dc).T
        rel_state = jnp.broadcast_to(jnp.pad(rel_ada, (0, d.relp - d.num_rel), constant_values=1.0), (8, d.relp))

        head_ids = (head_idx[0] * 2).reshape(-1)
        own_tail_ids = (tail_idx[0] * 2).reshape(-1)
        local = neg_idx - me * d.rows
        owned = (local >= 0) & (local < d.rows)
        neg_all = jnp.pad(jnp.where(owned, local, d.rows) * 2, ((0, 0), (0, d.negp - d.neg)), constant_values=2 * d.rows)
        place = lax.broadcasted_iota(I32, neg_all.shape, 1)
        key = jnp.where(neg_all < 2 * d.rows, place, place + d.negp)
        key, neg_rows = lax.sort((key, neg_all), dimension=1, num_keys=1)
        neg_src = key % d.negp * 2
        counts = jnp.sum(owned.astype(I32), axis=1)
        rel_ids = rel_idx[0].reshape(d.rounds * d.nch, CHUNK)
        weight = edge_mask[0].astype(F32).reshape(d.rounds * d.nch, CHUNK)
        neg_rows, neg_src = neg_rows.reshape(-1), neg_src.reshape(-1)
        table, head_ids, counts, neg_rows, neg_src, own_tail_ids = lax.optimization_barrier(
            (table, head_ids, counts, neg_rows, neg_src, own_tail_ids))

        own_lists = [counts, head_ids, own_tail_ids, neg_rows, neg_src]
        rows_in = table_step(d, None, 0, None, own_lists, None, table)
        losses = []
        for s in range(d.rounds):
            if s == 0:
                res = bucket_step(d, s, rows_in, rel_t, rel_state, rel_ids, rel_ids, weight, (own_tail_ids, rel_ids))
                rel_ids_p, tail_ids = res[6:]
                lists = [counts, head_ids, tail_ids, neg_rows, neg_src]
            else:
                res = bucket_step(d, s, rows_in, rel_t, rel_state, rel_ids, rel_ids_p, weight, ())
            hg, tg, ng, rel_t, rel_state, loss = res[:6]
            losses.append(loss)
            new = s + 1 if s + 1 < d.rounds else None
            table, *rows_in = table_step(d, s, new, own_lists if s == 0 else lists, lists, (hg, tg, ng), table)
        loss = jnp.sum(jnp.stack(losses), axis=(1, 2)) / d.edges
        emb, ada = unpack(d, table)
        rel_out = rel_t.T.reshape(d.relp, 2, d.hp)[:d.num_rel, :, :d.half].reshape(d.num_rel, d.dim)
        return emb, ada, rel_out, rel_state[0, :d.num_rel], loss[None, :]

    return jax.shard_map(device_fn, mesh=mesh,
                         in_specs=(row_spec, flat_spec, rel_spec, state_spec, edge_spec, edge_spec, edge_spec, edge_spec, rel_spec),
                         out_specs=(row_spec, flat_spec, rel_spec, state_spec, row_spec), check_vma=False)
```

```python
import functools

import jax
import jax.numpy as jnp
from jax import lax
from jax.experimental import pallas as pl
from jax.experimental.pallas import tpu as pltpu
from jax.sharding import PartitionSpec as P

LEARN_RATE = 0.05
ADA_EPS = 1e-10
LANES = 128
CHUNK = 256
PACK_ROWS = 1024
QUERY_GROUP, SCORE_GROUP, HEAD_GROUP, ROWS_GROUP, TAIL_GROUP = 2, 2, 2, 4, 2
TAILS_FIRST, TAILS_SECOND = 0, 2
AHEAD = 2
HEAD_SENDS = {0: (0, 2, 3, 4, 5, 7, 8), **{k: (2, 8, 8, 8, 8, 8, 8) for k in (1, 2, 3, 6, 7, 8)}}
F32, BF16, I32 = jnp.float32, jnp.bfloat16, jnp.int32
MESH = pl.DeviceIdType.MESH
VMEM = pltpu.VMEM


def round_up(value, multiple):
    return -(-value // multiple) * multiple


class Dims:
    def __init__(self, mesh, ent_emb, rel_emb, head_idx, neg_idx):
        self.ent = mesh.shape['ent']
        self.chips = self.ent // 2
        side = max(round(self.chips ** 0.5), 1)
        hops = lambda k: min(k % side, side - k % side) + min(k // side, side - k // side)
        self.far_first = sorted(range(1, self.chips), key=lambda k: -hops(k))
        self.rows, self.dim = ent_emb.shape
        self.half = self.dim // 2
        self.hp = round_up(self.half, 8)
        self.dc = 2 * self.hp
        self.num_rel = rel_emb.shape[0]
        self.relp = round_up(self.num_rel, LANES)
        self.rounds, self.edges = head_idx.shape[1:]
        self.nch = self.edges // CHUNK
        self.neg = neg_idx.shape[1]
        self.negp = round_up(self.neg, self.ent * 16)
        self.negc = self.negp // self.ent
        self.cols = (self.relp + self.negp) // LANES
        self.tiles = self.dc // 8 * self.cols
        self.tpd = -(-self.tiles // self.ent)
        self.trows = 2 * self.rows + 16


def nt_dot(lhs, rhs):
    return lax.dot_general(lhs, rhs, (((1,), (1,)), ((), ())), preferred_element_type=F32)


def nn_dot(lhs, rhs):
    return jnp.dot(lhs, rhs, preferred_element_type=F32)


def split3(x):
    hi = x.astype(BF16)
    rest = x - hi.astype(F32)
    mid = rest.astype(BF16)
    lo = (rest - mid.astype(F32)).astype(BF16)
    return hi, mid, lo


def iota(shape, dim):
    return lax.broadcasted_iota(I32, shape, dim)


def eye(n):
    return jnp.where(iota((n, n), 0) == iota((n, n), 1), 1.0, 0.0).astype(BF16)


def compact_sel(dims, out_rows):
    c = iota((out_rows, 2 * LANES), 0)
    lane = iota((out_rows, 2 * LANES), 1)
    src = jnp.where(c < dims.hp, c, c - dims.hp + LANES)
    return jnp.where((lane == src) & (c < dims.dc), 1.0, 0.0).astype(BF16)


def pack_kernel(half, last, e_ref, g_ref, o_ref):
    step = pl.program_id(0)
    row = iota((LANES, LANES), 0)
    low = half // 8 * 8
    gap = jnp.zeros((LANES - round_up(half, 8), LANES), F32)

    @pl.when(step < last)
    def _():
        for i in range(PACK_ROWS // LANES):
            cols = pl.ds(i * LANES, LANES)
            re = jnp.concatenate([e_ref[pl.ds(0, round_up(half, 8)), cols], gap], axis=0)
            re = jnp.where(row < half, re, 0.0)
            im = jnp.concatenate([e_ref[pl.ds(low, 2 * half - low), cols], jnp.zeros((LANES - (2 * half - low), LANES), F32)], axis=0)
            if half > low:
                im = pltpu.roll(im, LANES - (half - low), 0)
            im = jnp.where(row < half, im, 0.0)
            im = jnp.where(row == LANES - 1, g_ref[pl.ds(i, 1), :], im)
            o_ref[pl.ds(2 * i * LANES, LANES, stride=2), :] = jnp.transpose(re)
            o_ref[pl.ds(2 * i * LANES + 1, LANES, stride=2), :] = jnp.transpose(im)

    @pl.when(step == last)
    def _():
        o_ref[...] = jnp.zeros_like(o_ref)


def pack(dims, emb, ada):
    blocks = dims.rows // PACK_ROWS
    return pl.pallas_call(
        functools.partial(pack_kernel, dims.half, blocks),
        grid=(blocks + 1,),
        out_shape=jax.ShapeDtypeStruct((dims.trows, LANES), F32),
        in_specs=[pl.BlockSpec((dims.dim, PACK_ROWS), lambda i: (0, jnp.minimum(i, blocks - 1))),
                  pl.BlockSpec((PACK_ROWS // LANES, LANES), lambda i: (jnp.minimum(i, blocks - 1), 0))],
        out_specs=pl.BlockSpec((2 * PACK_ROWS, LANES), lambda i: (i, 0)),
        compiler_params=pltpu.CompilerParams(vmem_limit_bytes=16 << 20),
        name='pack')(emb.T, ada.reshape(dims.rows // LANES, LANES))


def unpack_kernel(half, t_ref, e_ref, g_ref):
    low = half // 8 * 8
    high = round_up(half, 8)
    for i in range(PACK_ROWS // LANES):
        cols = pl.ds(i * LANES, LANES)
        re = jnp.transpose(t_ref[pl.ds(2 * i * LANES, LANES, stride=2), :])
        im = jnp.transpose(t_ref[pl.ds(2 * i * LANES + 1, LANES, stride=2), :])
        g_ref[pl.ds(i, 1), :] = im[LANES - 1:]
        e_ref[pl.ds(0, low), cols] = re[:low]
        if half > low:
            im = pltpu.roll(im, half - low, 0)
            e_ref[pl.ds(low, 8), cols] = jnp.where(iota((8, LANES), 0) < half - low, re[low:high], im[:8])
            e_ref[pl.ds(high, 2 * half - high), cols] = im[8:8 + 2 * half - high]
        else:
            e_ref[pl.ds(half, half), cols] = im[:half]


def unpack(dims, table):
    blocks = dims.rows // PACK_ROWS
    emb, ada = pl.pallas_call(
        functools.partial(unpack_kernel, dims.half),
        grid=(blocks,),
        out_shape=[jax.ShapeDtypeStruct((dims.dim, dims.rows), F32),
                   jax.ShapeDtypeStruct((dims.rows // LANES, LANES), F32)],
        in_specs=[pl.BlockSpec((2 * PACK_ROWS, LANES), lambda i: (i, 0))],
        out_specs=[pl.BlockSpec((dims.dim, PACK_ROWS), lambda i: (0, i)),
                   pl.BlockSpec((PACK_ROWS // LANES, LANES), lambda i: (i, 0))],
        compiler_params=pltpu.CompilerParams(vmem_limit_bytes=16 << 20),
        name='unpack')(table)
    return emb.T, ada.reshape(dims.rows)


UNROLL_SCATTER = 16
UNROLL_GATHER = 64
UNROLL_NEG = 8
CONVERT_GROUP = 4
UPDATE_ROWS = 512


def table_kernel(dims, old, new, *refs):
    refs = list(refs)
    update_rows, gather_next = old is not None, new is not None

    def take(n):
        taken = refs[:n]
        del refs[:n]
        return taken
    edges, negp = dims.edges, dims.negp
    sources, lists = [], []
    if update_rows:
        old_count, = take(1)
        sources += take(4)
    if gather_next:
        new_count, = take(1)
        sources += take(4)
    if update_rows:
        head_g, tail_g, neg_g = take(3)
    table_in, = take(1)
    table, = take(1) if update_rows else (table_in,)
    if gather_next:
        tail_out, head_out, neg_out = take(3)
    lists = take(len(sources))
    sem, = take(1)
    if update_rows:
        acc_a, acc_b = take(2)
    steps = [old] * 4 * (old is not None) + [new] * 4 * (new is not None)
    copies = [pltpu.make_async_copy(src.at[pl.ds(step * dst.shape[0], dst.shape[0])], dst, sem.at[k])
              for k, (src, dst, step) in enumerate(zip(sources, lists, steps))]
    for copy in copies:
        copy.start()
    if update_rows:
        head_i, tail_i, neg_i, src_i = lists[:4]
        table_update(dims, copies, old_count[old], head_i, tail_i, neg_i, src_i, head_g, tail_g, neg_g, table_in, table, acc_a, acc_b)
    else:
        for copy in copies:
            copy.wait()
    if gather_next:
        head_i, tail_i, neg_i, src_i = lists[-4:]
        for ids, out in ((tail_i, tail_out), (head_i, head_out)):
            def gather(c, _):
                for u in range(UNROLL_GATHER):
                    k = c * UNROLL_GATHER + u
                    out[pair(k), :] = table[at(ids, k), :]
                return 0
            lax.fori_loop(0, edges // UNROLL_GATHER, gather, 0)

        neg_out[...] = jnp.zeros_like(neg_out)

        def gather_neg(c, _):
            rows = [table[at(neg_i, c * UNROLL_NEG + u), :] for u in range(UNROLL_NEG)]
            for u in range(UNROLL_NEG):
                neg_out[at(src_i, c * UNROLL_NEG + u), :] = rows[u]
            return 0
        lax.fori_loop(0, (new_count[new] + UNROLL_NEG - 1) // UNROLL_NEG, gather_neg, 0)


def table_update(dims, copies, count, head_i, tail_i, neg_i, src_i, head_g, tail_g, neg_g, table_in, table, acc_a, acc_b):
    edges = dims.edges

    def zero(c, _):
        rows = pl.ds(pl.multiple_of(c * 256, 256), 256)
        acc_a[rows, :] = jnp.zeros((256, LANES), F32)
        acc_b[rows, :] = jnp.zeros((256, LANES), F32)
        return 0
    lax.fori_loop(0, 2 * dims.rows // 256, zero, 0)
    for copy in copies:
        copy.wait()

    def scatter(c, _):
        for u in range(0, UNROLL_SCATTER, 2):
            k = c * UNROLL_SCATTER + u
            h0, h1, t0, t1 = at(head_i, k), at(head_i, k + 1), at(tail_i, k), at(tail_i, k + 1)
            a0 = acc_a[h0, :] + head_g[pair(k), :]
            b0 = acc_b[t0, :] + tail_g[pair(k), :]
            a1 = jnp.where(head_i[k] == head_i[k + 1], a0, acc_a[h1, :]) + head_g[pair(k + 1), :]
            b1 = jnp.where(tail_i[k] == tail_i[k + 1], b0, acc_b[t1, :]) + tail_g[pair(k + 1), :]
            acc_a[h0, :] = a0
            acc_b[t0, :] = b0
            acc_a[h1, :] = a1
            acc_b[t1, :] = b1
        return 0
    lax.fori_loop(0, edges // UNROLL_SCATTER, scatter, 0)

    def scatter_neg(c, _):
        for u in range(0, UNROLL_NEG, 2):
            k = c * UNROLL_NEG + u
            h, t = at(neg_i, k), at(neg_i, k + 1)
            new_a = acc_a[h, :] + neg_g[at(src_i, k), :]
            new_b = acc_b[t, :] + neg_g[at(src_i, k + 1), :]
            acc_a[h, :] = new_a
            acc_b[t, :] = new_b
        return 0
    lax.fori_loop(0, (count + UNROLL_NEG - 1) // UNROLL_NEG, scatter_neg, 0)

    lane = iota((UPDATE_ROWS, LANES), 1)

    def update(c, _):
        base = pl.multiple_of(c * 2 * UPDATE_ROWS, 2 * UPDATE_ROWS)
        re = pl.ds(base, UPDATE_ROWS, stride=2)
        im = pl.ds(base + 1, UPDATE_ROWS, stride=2)
        g_re = acc_a[re, :] + acc_b[re, :]
        g_im = acc_a[im, :] + acc_b[im, :]
        e_re, e_im = table_in[re, :], table_in[im, :]
        part = (g_re * g_re + g_im * g_im) * (1.0 / dims.dim)
        part = jnp.where(lane == LANES - 1, e_im, part)
        state = jnp.sum(part, axis=1, keepdims=True)
        rate = LEARN_RATE * lax.rsqrt(state + ADA_EPS)
        table[re, :] = e_re - rate * g_re
        table[im, :] = jnp.where(lane == LANES - 1, state, e_im - rate * g_im)
        return 0
    lax.fori_loop(0, dims.rows // UPDATE_ROWS, update, 0)
    table[pl.ds(2 * dims.rows, 16), :] = jnp.zeros((16, LANES), F32)


def pair(k):
    return pl.ds(pl.multiple_of(2 * k, 2), 2)


def at(ref, k):
    return pl.ds(pl.multiple_of(ref[k], 2), 2)


def table_step(dims, old, new, old_lists, new_lists, grads, table):
    vm = pl.BlockSpec(memory_space=VMEM)
    smem = pl.BlockSpec(memory_space=pltpu.SMEM)
    anys = pl.BlockSpec(memory_space=pl.ANY)
    sizes = (dims.edges, dims.edges, dims.negp, dims.negp)
    operands, in_specs, outs, scratch, aliases = [], [], [], [], {}
    for step, lists in ((old, old_lists), (new, new_lists)):
        if step is not None:
            operands += lists
            in_specs += [smem] + [anys] * 4
            scratch += [pltpu.SMEM((n,), I32) for n in sizes]
    scratch.append(pltpu.SemaphoreType.DMA((len(scratch),)))
    if old is not None:
        operands += grads
        in_specs += [vm] * 3
        aliases = {len(operands): 0}
        outs.append(jax.ShapeDtypeStruct((dims.trows, LANES), F32))
        scratch += [VMEM((dims.trows, LANES), F32)] * 2
    operands.append(table)
    in_specs.append(vm)
    if new is not None:
        outs += [jax.ShapeDtypeStruct((2 * n, LANES), F32) for n in (dims.edges, dims.edges, dims.negp)]
    return pl.pallas_call(
        functools.partial(table_kernel, dims, old, new),
        out_shape=outs, in_specs=in_specs, out_specs=[vm] * len(outs), scratch_shapes=scratch,
        input_output_aliases=aliases, name='table',
        compiler_params=pltpu.CompilerParams(vmem_limit_bytes=24 << 20))(*operands)


def bucket_kernel(dims, s, *refs):
    (head_rows_in, tail_rows_in, neg_rows_in, rel_t, rel_state, rel_ids, rel_ids_p, weight), refs = refs[:8], refs[8:]
    if s == 0:
        (tail_x, rel_x), refs = refs[:2], refs[2:]
    (head_g, tail_g, neg_g, rel_t_out, rel_state_out, loss), refs = refs[:6], refs[6:]
    if s == 0:
        (rel_x_out, tail_x_out), refs = refs[:2], refs[2:]
        (x_ss, x_rs), refs = refs[:2], refs[2:]
    (head, tail, neg, tail_r, head_r, dp_s, dp_r, splits, q_all, r_all, qb, ex, top_s, sum_s, neg_p, neg_half, neg_buf, neg_acc, neg_all, neg_t,
     acc_rel, acc_neg, head_c, x_ar, p_ar, half_ar, buf_ar, acc_ar, o_ar,
     tail_ss, tail_rs, head_ss, head_rs, one_s, one_r, rs_s, rs_r, ag_s, ag_r, rs2_s, rs2_r, ag2_s, ag2_r) = refs
    ent, chips, hp, dc, nch = dims.ent, dims.chips, dims.hp, dims.dc, dims.nch
    me = lax.axis_index('ent')
    core, chip = lax.rem(me, 2), me // 2
    partner = me + 1 - 2 * core
    dst_t = lax.rem(me + ent - s, ent)
    dst_h = lax.rem(me + s, ent)

    def dev(d):
        return {'ent': d}

    def peer(k):
        return lax.rem(chip + k, chips) * 2 + core

    def remote(src, dst, ss, rs, d):
        return pltpu.make_async_remote_copy(src_ref=src, dst_ref=dst, send_sem=ss, recv_sem=rs, device_id=dev(d), device_id_type=MESH)

    def loop(lo, hi, fn):
        def body(k, _):
            fn(k)
            return 0
        lax.fori_loop(lo, hi, body, 0)

    def chunks(group, fn):
        loop(0, nch // group, lambda k: fn([k * group + i for i in range(group)]))

    barrier = pltpu.get_barrier_semaphore()

    def signal(d):
        pl.semaphore_signal(barrier, inc=1, device_id=dev(d), device_id_type=MESH)
    if s:
        signal(dst_t)
        signal(dst_h)
        others = 2
    else:
        loop(1, dims.rounds, lambda k: signal(lax.rem(me + ent - k, ent)))
        others = dims.rounds - 1
    loop(1, chips, lambda k: signal(peer(k)))
    signal(partner)

    def one_hot(ids_ref, c):
        ids = ids_ref[pl.ds(s * nch + c, 1), :]
        return jnp.where(iota((dims.relp, CHUNK), 0) == ids, 1.0, 0.0).astype(BF16)

    def rel_rows(hot):
        r = nn_dot(splits[...], hot)
        return (r[:dc] + r[dc:2 * dc]) + r[2 * dc:]

    def queries(rows, r):
        x = rows.astype(F32)
        h_re, h_im, r_re, r_im = x[:hp], x[hp:], r[:hp], r[hp:]
        return jnp.concatenate([h_re * r_re - h_im * r_im, h_re * r_im + h_im * r_re], axis=0)

    def rel_query(cs):
        for c in cs:
            r_all[c] = rel_rows(one_hot(rel_ids, c))

    def head_query(cs):
        for c in cs:
            q = queries(head[c], r_all[c])
            q_all[c] = q
            qb[c, pl.ds(0, dc), :] = q.astype(BF16)

    ident = eye(CHUNK)
    for c in range(nch):
        qb[c, pl.ds(dc, 2 * LANES - dc), :] = jnp.zeros((2 * LANES - dc, CHUNK), BF16)
    acc_rel[...] = jnp.zeros_like(acc_rel)
    acc_neg[...] = jnp.zeros_like(acc_neg)
    loss[...] = jnp.zeros_like(loss)
    sel = compact_sel(dims, 2 * LANES)

    def edge_rows(ref, c):
        base = pl.multiple_of(c * 2 * CHUNK, 2 * CHUNK)
        re = ref[pl.ds(base, CHUNK, stride=2), :]
        im = ref[pl.ds(base + 1, CHUNK, stride=2), :]
        return jnp.concatenate([re.astype(BF16), im.astype(BF16)], axis=1)

    def convert(ref, out):
        def group(cs):
            for c in cs:
                out[c] = nt_dot(sel[:dc], edge_rows(ref, c)).astype(BF16)
        chunks(CONVERT_GROUP, group)
    per = CHUNK // dims.negc
    for c in range(dims.negp // CHUNK):
        neg[c * per // chips, pl.ds(c * per % chips, per)] = nt_dot(edge_rows(neg_rows_in, c), sel).astype(BF16).reshape(per, dims.negc, 2 * LANES)
    convert(tail_rows_in, tail)

    pl.semaphore_wait(barrier, chips + others)

    def tail_copy(c):
        return remote(tail.at[c], tail_r.at[c], tail_ss.at[c], tail_rs.at[c], dst_t)

    def head_copy(c):
        return remote(head.at[c], head_r.at[c], head_ss.at[c], head_rs.at[c], dst_h)

    def send_tails(lo, hi):
        if s:
            loop(lo, hi, lambda c: tail_copy(c).start())

    def send_heads(lo, hi):
        if s and hi > lo:
            loop(lo, hi, lambda c: head_copy(c).start())
    plan = (0,) + HEAD_SENDS.get(s, HEAD_SENDS[0])
    late = s > 0 and plan[2] < nch

    def send_heads_at(point):
        if point < 2:
            send_heads(plan[point], plan[point + 1])
        elif s:
            for c in range(plan[point], plan[point + 1]):
                if c >= AHEAD:
                    head_copy(c - AHEAD).wait_send()
                head_copy(c).start()
    if s:
        tail_in, head_in, dp_in = tail_r, head_r, dp_r
    else:
        tail_in, head_in, dp_in = tail, head, dp_s

    send_tails(0, TAILS_FIRST)
    neg_pair = remote(neg.at[1 - core], neg_p, one_s.at[0], one_r.at[0], partner)
    neg_pair.start()
    neg_pair.wait_recv()
    neg_half[...] = neg[core] + neg_p[...]

    def rs_neg(k):
        return remote(neg_half.at[lax.rem(chip + k, chips)], neg_buf.at[k], rs_s.at[k], rs_r.at[k], peer(k))
    for k in dims.far_first:
        rs_neg(k).start()
    send_tails(TAILS_FIRST, TAILS_SECOND)
    convert(head_rows_in, head)
    send_heads_at(0)
    neg_acc[...] = neg_half[chip]

    def take_neg(k):
        rs_neg(k).wait_recv()
        neg_acc[...] = neg_acc[...] + neg_buf[k]
    loop(1, chips, take_neg)

    def ag_neg(k):
        return remote(neg_acc, neg_all.at[core, chip], ag_s.at[k], ag_r.at[k], peer(k))
    for k in dims.far_first:
        ag_neg(k).start()
    send_tails(TAILS_SECOND, nch)
    send_heads_at(1)
    if s == 0:
        def rel_copy(k):
            rows = pl.ds(pl.multiple_of(k * nch, nch), nch)
            return remote(rel_x.at[rows], rel_x_out.at[rows], x_ss.at[0, k], x_rs.at[0, k], lax.rem(me + k, ent))

        def id_copy(k):
            rows = pl.ds(k * dims.edges, dims.edges)
            return remote(tail_x.at[rows], tail_x_out.at[rows], x_ss.at[1, k], x_rs.at[1, k], lax.rem(me + k, ent))
        loop(1, dims.rounds, lambda k: rel_copy(k).start())
        for k in range(1, dims.rounds):
            id_copy(k).start()
        rel_x_out[pl.ds(0, nch), :] = rel_x[pl.ds(0, nch), :]
        tail_x_out[pl.ds(0, dims.edges)] = tail_x[pl.ds(0, dims.edges)]
    for i, part in enumerate(split3(rel_t[...])):
        splits[pl.ds(i * dc, dc), :] = part
    chunks(QUERY_GROUP, rel_query)
    chunks(QUERY_GROUP, head_query)
    neg_all[core, chip] = neg_acc[...]
    loop(1, chips, lambda k: ag_neg(k).wait_recv())
    neg_pair2 = remote(neg_all.at[core], neg_all.at[core], one_s.at[1], one_r.at[1], partner)
    neg_pair2.start()
    neg_pair2.wait_recv()
    neg_t[...] = nt_dot(eye(2 * LANES), neg_all[...].reshape(dims.negp, 2 * LANES)).astype(BF16)

    main = dims.neg // 16 * 16

    def score(cs):
        for c in cs:
            scores = nn_dot(neg_all[...].reshape(dims.negp, 2 * LANES), qb[c])
            body = scores[:main]
            top = jnp.max(body, axis=0, keepdims=True)
            if main < dims.negp:
                rest = jnp.where(iota((dims.negp - main, CHUNK), 0) < dims.neg - main, scores[main:], -1e30)
                top = jnp.maximum(top, jnp.max(rest, axis=0, keepdims=True))
            e_body = jnp.exp(body - top)
            ex[c, pl.ds(0, main), :] = e_body
            total = jnp.sum(e_body, axis=0, keepdims=True)
            if main < dims.negp:
                e_rest = jnp.exp(rest - top)
                ex[c, pl.ds(main, dims.negp - main), :] = e_rest
                total = total + jnp.sum(e_rest, axis=0, keepdims=True)
            top_s[pl.ds(c, 1), :] = top
            sum_s[pl.ds(c, 1), :] = total
    chunks(SCORE_GROUP, score)

    def head_side(cs):
        if s:
            for c in cs:
                tail_copy(c).wait_recv()
        lost, neg_q, neg_d, rel_parts, rel_hot = [], [], [], [], []
        for c in cs:
            t = tail_in[c].astype(F32)
            pos = jnp.sum(q_all[c] * t, axis=0, keepdims=True)
            neg_top = top_s[pl.ds(c, 1), :]
            top = jnp.maximum(pos, neg_top)
            pos_exp = jnp.exp(pos - top)
            scale = jnp.exp(neg_top - top)
            norm = pos_exp + scale * sum_s[pl.ds(c, 1), :]
            w = weight[pl.ds(s * nch + c, 1), :]
            lost.append(w * (top + jnp.log(norm) - pos))
            dp = w * (pos_exp / norm - 1.0)
            dp_s[pl.ds(c, 1), :] = dp
            ds = (ex[c] * (w * scale / norm)).astype(BF16)
            g = dp * t + nn_dot(neg_t[pl.ds(0, dc), :], ds)
            neg_q.append(qb[c, pl.ds(0, dc), :])
            neg_d.append(ds)
            g_re, g_im = g[:hp], g[hp:]
            r = r_all[c]
            r_re, r_im = r[:hp], r[hp:]
            head_c[c] = jnp.concatenate([g_re * r_re + g_im * r_im, g_im * r_re - g_re * r_im], axis=0)
            h = head[c].astype(F32)
            h_re, h_im = h[:hp], h[hp:]
            rel_g = jnp.concatenate([g_re * h_re + g_im * h_im, g_im * h_re - g_re * h_im], axis=0)
            rel_parts.append(jnp.concatenate(split3(rel_g), axis=0))
            rel_hot.append(one_hot(rel_ids, c))
        loss[pl.ds(0, 1), :] += sum(lost)
        acc_neg[...] += nt_dot(jnp.concatenate(neg_q, axis=1), jnp.concatenate(neg_d, axis=1))
        part = nt_dot(jnp.concatenate(rel_parts, axis=1), jnp.concatenate(rel_hot, axis=1))
        acc_rel[...] += (part[:dc] + part[dc:2 * dc]) + part[2 * dc:]
    chunks(HEAD_GROUP, head_side)

    if s:
        dp_copy = remote(dp_s, dp_r, one_s.at[2], one_r.at[2], dst_h)
        dp_copy.start()

    def tile_place(t):
        d, j = t // dims.tpd, t % dims.tpd
        return d // chips, d % chips, j
    rel_cols = dims.relp // LANES
    for t in range(dims.tpd * ent):
        i, j = t // dims.cols, t % dims.cols
        if t >= dims.tiles:
            x_ar[tile_place(t)] = jnp.zeros((8, LANES), F32)
        elif j < rel_cols:
            x_ar[tile_place(t)] = acc_rel[pl.ds(8 * i, 8), pl.ds(j * LANES, LANES)]
        else:
            x_ar[tile_place(t)] = acc_neg[pl.ds(8 * i, 8), pl.ds((j - rel_cols) * LANES, LANES)]

    ar_pair = remote(x_ar.at[1 - core], p_ar, one_s.at[3], one_r.at[3], partner)
    ar_pair.start()
    send_heads_at(2)

    def rows_of(cols):
        gap = jnp.zeros((LANES - hp, CHUNK), F32)
        x = jnp.concatenate([cols[:hp], gap, cols[hp:], gap], axis=0)
        return nt_dot(jnp.concatenate([ident] * 3, axis=1), jnp.concatenate(split3(x), axis=1))

    def put_rows(out, c, rows):
        base = pl.multiple_of(c * 2 * CHUNK, 2 * CHUNK)
        out[pl.ds(base, CHUNK, stride=2), :] = rows[:, :LANES]
        out[pl.ds(base + 1, CHUNK, stride=2), :] = rows[:, LANES:]

    def head_rows(cs):
        for c in cs:
            put_rows(head_g, c, rows_of(head_c[c]))

    def tail_side(cs):
        if s:
            for c in cs:
                head_copy(c).wait_recv()
        for c in cs:
            q = queries(head_in[c], rel_rows(one_hot(rel_ids_p, c)))
            put_rows(tail_g, c, rows_of(dp_in[pl.ds(c, 1), :] * q))

    ar_pair.wait_recv()
    half_ar[...] = x_ar[core] + p_ar[...]

    def rs_ar(k):
        return remote(half_ar.at[lax.rem(chip + k, chips)], buf_ar.at[k], rs2_s.at[k], rs2_r.at[k], peer(k))
    for k in dims.far_first:
        rs_ar(k).start()
    send_heads_at(3)
    chunks(ROWS_GROUP, head_rows)
    send_heads_at(4)
    acc_ar[...] = half_ar[chip]

    def take_ar(k):
        rs_ar(k).wait_recv()
        acc_ar[...] += buf_ar[k]
    loop(1, chips, take_ar)

    def ag_ar(k):
        return remote(acc_ar, o_ar.at[core, chip], ag2_s.at[k], ag2_r.at[k], peer(k))
    for k in dims.far_first:
        ag_ar(k).start()
    send_heads_at(5)
    o_ar[core, chip] = acc_ar[...]
    def tail_gradients():
        if s:
            dp_copy.wait_recv()
        chunks(TAIL_GROUP, tail_side)
    if not late:
        tail_gradients()
    loop(1, chips, lambda k: ag_ar(k).wait_recv())
    ar_pair2 = remote(o_ar.at[core], o_ar.at[core], one_s.at[4], one_r.at[4], partner)
    ar_pair2.start()
    send_heads_at(6)
    ar_pair2.wait_recv()

    for t in range(dims.tiles):
        i, j = t // dims.cols, t % dims.cols
        if j < rel_cols:
            acc_rel[pl.ds(8 * i, 8), pl.ds(j * LANES, LANES)] = o_ar[tile_place(t)]
        else:
            acc_neg[pl.ds(8 * i, 8), pl.ds((j - rel_cols) * LANES, LANES)] = o_ar[tile_place(t)]
    g = acc_rel[...]
    state = rel_state[...] + jnp.sum(g * g, axis=0, keepdims=True) * (1.0 / dims.dim)
    rel_state_out[...] = state
    rel_t_out[...] = rel_t[...] - LEARN_RATE * g / jnp.sqrt(state[:1] + ADA_EPS)
    for c in range(dims.negp // CHUNK):
        put_rows(neg_g, c, rows_of(acc_neg[:, pl.ds(c * CHUNK, CHUNK)]))
    if late:
        tail_gradients()

    neg_pair.wait_send()
    neg_pair2.wait_send()
    ar_pair.wait_send()
    ar_pair2.wait_send()
    if s:
        dp_copy.wait_send()

        loop(0, nch, lambda c: tail_copy(c).wait_send())
        for c in range(nch):
            if plan[2] == nch or c >= nch - AHEAD or c < plan[2] - AHEAD:
                head_copy(c).wait_send()

    if s == 0:
        def moved(k):
            rel_copy(k).wait()
        loop(1, dims.rounds, moved)
        for k in range(1, dims.rounds):
            id_copy(k).wait()

    def sent_peers(k):
        rs_neg(k).wait_send()
        ag_neg(k).wait_send()
        rs_ar(k).wait_send()
        ag_ar(k).wait_send()
    loop(1, chips, sent_peers)


def bucket_step(dims, s, rows_in, rel_t, rel_state, rel_ids, rel_ids_p, weight, extra):
    d = dims
    vm = pl.BlockSpec(memory_space=VMEM)
    sds = jax.ShapeDtypeStruct
    dma = pltpu.SemaphoreType.DMA
    outs = [sds((2 * d.edges, LANES), F32), sds((2 * d.edges, LANES), F32), sds((2 * d.negp, LANES), F32),
            sds((d.dc, d.relp), F32), sds((8, d.relp), F32), sds((8, CHUNK), F32)]
    if extra:
        outs += [sds(extra[1].shape, I32), sds(extra[0].shape, I32)]
    tail, head, neg = rows_in
    rows = VMEM((d.nch, d.dc, CHUNK), BF16)
    wide = VMEM((d.nch, d.dc, CHUNK), F32)
    line = VMEM((d.nch, CHUNK), F32)
    neg_part = VMEM((d.chips, d.negc, 2 * LANES), BF16)
    ar_part = VMEM((d.chips, d.tpd, 8, LANES), F32)
    scratch = [dma((2, d.rounds))] * 2 if extra else []
    scratch += [rows, rows, VMEM((2, d.chips, d.negc, 2 * LANES), BF16), rows, rows, line, line,
                VMEM((3 * d.dc, d.relp), BF16), wide, wide, VMEM((d.nch, 2 * LANES, CHUNK), BF16),
                VMEM((d.nch, d.negp, CHUNK), F32), line, line,
                neg_part, neg_part, neg_part, VMEM((d.negc, 2 * LANES), BF16),
                VMEM((2, d.chips, d.negc, 2 * LANES), BF16), VMEM((2 * LANES, d.negp), BF16),
                VMEM((d.dc, d.relp), F32), VMEM((d.dc, d.negp), F32), wide,
                VMEM((2, d.chips, d.tpd, 8, LANES), F32), ar_part, ar_part, ar_part,
                VMEM((d.tpd, 8, LANES), F32), VMEM((2, d.chips, d.tpd, 8, LANES), F32),
                dma((d.nch,)), dma((d.nch,)), dma((d.nch,)), dma((d.nch,)), dma((5,)), dma((5,))]
    scratch += [dma((d.chips,))] * 8
    return pl.pallas_call(
        functools.partial(bucket_kernel, d, s), out_shape=outs,
        in_specs=[vm] * (8 + len(extra)), out_specs=[vm] * len(outs),
        scratch_shapes=scratch, name=f'bucket_{s}',
        compiler_params=pltpu.CompilerParams(collective_id=s, has_side_effects=True, vmem_limit_bytes=36 << 20),
    )(head, tail, neg, rel_t, rel_state, rel_ids, rel_ids_p, weight, *extra)


def solution(mesh):
    row_spec = P(('sweep', 'ent'), None)
    flat_spec = P(('sweep', 'ent'))
    rel_spec = P('sweep', None)
    state_spec = P('sweep')
    edge_spec = P(('sweep', 'ent'), None, None)

    def device_fn(ent_emb, ent_ada, rel_emb, rel_ada, head_idx, tail_idx, rel_idx, edge_mask, neg_idx):
        d = Dims(mesh, ent_emb, rel_emb, head_idx, neg_idx)
        me = lax.axis_index('ent')
        table = pack(d, ent_emb, ent_ada)
        rel = jnp.pad(rel_emb.reshape(d.num_rel, 2, d.half), ((0, d.relp - d.num_rel), (0, 0), (0, d.hp - d.half)))
        rel_t = rel.reshape(d.relp, d.dc).T
        rel_state = jnp.broadcast_to(jnp.pad(rel_ada, (0, d.relp - d.num_rel), constant_values=1.0), (8, d.relp))

        head_ids = (head_idx[0] * 2).reshape(-1)
        own_tail_ids = (tail_idx[0] * 2).reshape(-1)
        local = neg_idx - me * d.rows
        owned = (local >= 0) & (local < d.rows)
        neg_all = jnp.pad(jnp.where(owned, local, d.rows) * 2, ((0, 0), (0, d.negp - d.neg)), constant_values=2 * d.rows)
        place = lax.broadcasted_iota(I32, neg_all.shape, 1)
        key = jnp.where(neg_all < 2 * d.rows, place, place + d.negp)
        key, neg_rows = lax.sort((key, neg_all), dimension=1, num_keys=1)
        neg_src = key % d.negp * 2
        counts = jnp.sum(owned.astype(I32), axis=1)
        rel_ids = rel_idx[0].reshape(d.rounds * d.nch, CHUNK)
        weight = edge_mask[0].astype(F32).reshape(d.rounds * d.nch, CHUNK)
        neg_rows, neg_src = neg_rows.reshape(-1), neg_src.reshape(-1)
        table, head_ids, counts, neg_rows, neg_src, own_tail_ids = lax.optimization_barrier(
            (table, head_ids, counts, neg_rows, neg_src, own_tail_ids))

        own_lists = [counts, head_ids, own_tail_ids, neg_rows, neg_src]
        rows_in = table_step(d, None, 0, None, own_lists, None, table)
        losses = []
        for s in range(d.rounds):
            if s == 0:
                res = bucket_step(d, s, rows_in, rel_t, rel_state, rel_ids, rel_ids, weight, (own_tail_ids, rel_ids))
                rel_ids_p, tail_ids = res[6:]
                lists = [counts, head_ids, tail_ids, neg_rows, neg_src]
            else:
                res = bucket_step(d, s, rows_in, rel_t, rel_state, rel_ids, rel_ids_p, weight, ())
            hg, tg, ng, rel_t, rel_state, loss = res[:6]
            losses.append(loss)
            new = s + 1 if s + 1 < d.rounds else None
            table, *rows_in = table_step(d, s, new, own_lists if s == 0 else lists, lists, (hg, tg, ng), table)
        loss = jnp.sum(jnp.stack(losses), axis=(1, 2)) / d.edges
        emb, ada = unpack(d, table)
        rel_out = rel_t.T.reshape(d.relp, 2, d.hp)[:d.num_rel, :, :d.half].reshape(d.num_rel, d.dim)
        return emb, ada, rel_out, rel_state[0, :d.num_rel], loss[None, :]

    return jax.shard_map(device_fn, mesh=mesh,
                         in_specs=(row_spec, flat_spec, rel_spec, state_spec, edge_spec, edge_spec, edge_spec, edge_spec, rel_spec),
                         out_specs=(row_spec, flat_spec, rel_spec, state_spec, row_spec), check_vma=False)
```
